128 devices in a mesh: op: 4 (over z), row: 32 (over y, x, core).
Axes of the slice: x: 4, y: 4, z: 4, core: 2. Of those that a mesh axis runs over, the one named last changes fastest.
Arguments:
- wannier_ops: bfloat16 [2, 4000, 2, 128, 128], P(None, 'row'), may hold values from -0.09375 to 0.09375
- r_coords: int32 [4000, 3], P('row'), may hold values from -8 to 8
- degeneracy: int32 [4000], P('row'), may hold values from 1 to 4
- kpoints: int32 [256, 3], replicated, may hold values from 0 to 15
- bloch_vectors: bfloat16 [256, 2, 64, 128], P(('op', 'row')), may hold values from -0.375 to 0.375
Outputs:
- covariant: float32 [256, 2, 4096], P(('op', 'row'))
The draws below stay inside these ranges and needn't reach their ends.
Inputs may be any that keep to these rules, and one draw needn't show every extreme that they name: `r_coords`: these coordinates are small integers; a program may pack several of them into one int32 word when it moves them. `degeneracy`: these degeneracies are small integers; a program may pack several of them into one int32 word when it moves them.
All inputs are finite; a program needn't handle non-finite values.
Results may differ from the reference program's by a relative error of at most 0.0038.
Values may be sent and summed in bfloat16 or wider, within the bound.
A program may use at most 192 MiB of HBM per device.

```python
import math
import jax
import jax.numpy as jnp
from jax import lax

W = 128
NB = 64
GRID = 16
RMAX = 8
NR = 4000
K = 256


def place_ends(entries, rng, least, top_value):
    longest = entries.shape.index(max(entries.shape))
    spots = []
    for shift in (0, 1):
        where = [jax.random.randint(jax.random.fold_in(rng, axis), (), 0, length) for axis, length in enumerate(entries.shape)]
        where[longest] = (where[longest] + shift) % entries.shape[longest]
        spots.append(tuple(where))
    return entries.at[spots[0]].set(least).at[spots[1]].set(top_value)


def block_levels(key, dims, split, smallest, high):
    factor_of, own = 1.0, jax.random.fold_in(key, 6)
    for position, parts in split:
        heights = jnp.exp(jax.random.uniform(jax.random.fold_in(own, position), (parts,), jnp.float32, smallest / len(split), high / len(split)))
        factor_of = factor_of * jnp.repeat(heights, dims[position] // parts).reshape([-1 if axis == position else 1 for axis in range(len(dims))])
    return factor_of


def scatter_about(rng, shape, scale, most, split=(), kind=jnp.bfloat16):
    drawn = jax.random.normal(rng, shape, jnp.float32) * scale
    if len(split) > 0:
        drawn = block_levels(rng, shape, split, -0.22, 0.18) * drawn
    return jnp.clip(drawn, min=-most, max=most).astype(kind)


def setup_inputs(seed: int = 0) -> dict:
    key_of = jax.random.split(jax.random.key(seed), 6)
    wannier_ops = scatter_about(key_of[0], (2, NR, 2, W, W), NR ** -0.5, 0.09375, ((1, 32),))
    r_coords = place_ends(jax.random.randint(key_of[1], (NR, 3), -RMAX, RMAX + 1), jax.random.fold_in(key_of[1], 1), -RMAX, RMAX).astype(jnp.int32)
    degeneracy = place_ends(jax.random.randint(key_of[2], (NR,), 1, 5), jax.random.fold_in(key_of[2], 1), 1, 4).astype(jnp.int32)
    kpoints = place_ends(jax.random.randint(key_of[3], (K, 3), 0, GRID), jax.random.fold_in(key_of[3], 1), 0, GRID - 1).astype(jnp.int32)
    bloch_vectors = scatter_about(key_of[4], (K, 2, NB, W), (2 * W) ** -0.5, 0.375, ((0, 128),))
    return dict(wannier_ops=wannier_ops, r_coords=r_coords, degeneracy=degeneracy, kpoints=kpoints, bloch_vectors=bloch_vectors)


TWO_PI = 6.283185307179586
HIGH = lax.Precision.HIGHEST

def phase_parts(r_coords, degeneracy, kpoints):
    turns_int = lax.optimization_barrier(jnp.sum(r_coords[:, None, :] * kpoints[None, :, :], axis=2)) % GRID
    angles = turns_int.astype(jnp.float32) * (TWO_PI / GRID)
    weights = 1.0 / degeneracy.astype(jnp.float32)
    cosine = jnp.cos(angles) * weights[:, None]
    sine_part = jnp.sin(angles) * weights[:, None]
    along_x = (r_coords[:, 0].astype(jnp.float32) / RMAX)[:, None]
    return (cosine, sine_part, along_x)

def fourier(phase_re, phase_im, flat_ops):
    stacked = jnp.concatenate([phase_re, phase_im], axis=1)
    product_sum = lax.dot_general(stacked, flat_ops, (((0,), (0,)), ((), ())), preferred_element_type=jnp.float32)
    k_count = phase_re.shape[1]
    half_cols = flat_ops.shape[1] // 2
    real_part = product_sum[:k_count, :half_cols] - product_sum[k_count:, half_cols:]
    imag_part = product_sum[:k_count, half_cols:] + product_sum[k_count:, :half_cols]
    return (real_part, imag_part)

def complex_mul(form, left, right):

    def single(first, second):
        return jnp.einsum(form, first, second, precision=HIGH)
    return (single(left[0], right[0]) - single(left[1], right[1]), single(left[0], right[1]) + single(left[1], right[0]))

def rotate(op_pair, vec_pair):
    left_side = complex_mul('knm,kmp->knp', (vec_pair[0], -vec_pair[1]), op_pair)
    return complex_mul('knm,kpm->knp', left_side, vec_pair)

def covariant_form(ham, deriv, posit, posit_deriv):
    band_count = ham[0].shape[-1]
    factor = 1.0 / math.sqrt(band_count)
    form = 'kab,kbc->kac'
    a_d = complex_mul(form, posit, deriv)
    d_a = complex_mul(form, deriv, posit)
    h_a = complex_mul(form, ham, posit)
    a_h = complex_mul(form, posit, ham)
    g_real = posit_deriv[0] + factor * (h_a[0] + a_h[0] - (a_d[1] - d_a[1]))
    g_imag = posit_deriv[1] + factor * (h_a[1] + a_h[1] + (a_d[0] - d_a[0]))
    k_count = g_real.shape[0]
    return jnp.stack([g_real.reshape(k_count, -1), g_imag.reshape(k_count, -1)], axis=1)

def reference(wannier_ops, r_coords, degeneracy, kpoints, bloch_vectors):
    cosine, sine_part, along_x = phase_parts(r_coords, degeneracy, kpoints)
    vectors = bloch_vectors.astype(jnp.float32)
    vec_pair = (vectors[:, 0], vectors[:, 1])
    rotated = []
    for component_id in range(4):
        flat_ops = wannier_ops[component_id // 2].reshape(NR, 2 * W * W)
        if component_id % 2 == 1:
            phase_re = -along_x * sine_part
            phase_im = along_x * cosine
        else:
            phase_re = cosine
            phase_im = sine_part
        real_part, imag_part = fourier(phase_re.astype(jnp.bfloat16), phase_im.astype(jnp.bfloat16), flat_ops)
        rotated.append(rotate((real_part.reshape(K, W, W), imag_part.reshape(K, W, W)), vec_pair))
    return covariant_form(rotated[0], rotated[1], rotated[2], rotated[3])
```

```python
import functools

import jax
import jax.numpy as jnp
from jax import lax
from jax.experimental import pallas as pl
from jax.experimental.pallas import tpu as pltpu
from jax.sharding import PartitionSpec as P

MESH = pl.DeviceIdType.MESH
HIGH = lax.Precision.HIGHEST
F32 = jnp.float32
BF16 = jnp.bfloat16

NR_LOC = 125
HALVES = ((0, 64), (64, 61))
BANDS = 64
FACTOR = 1.0 / 8.0
S0, S1, S2, S3 = 0.392698743691337, -0.010092707352671412, 7.766394538597307e-05, -2.6791896176843414e-07


def nt(a, b, precision=None):
    return lax.dot_general(
        a, b, (((1,), (1,)), ((), ())), preferred_element_type=F32, precision=precision
    )


def mm(a, b, precision=None):
    return jnp.dot(a, b, preferred_element_type=F32, precision=precision)


def kernel(words_ref, kp_ref, v_ref, ops_ref, out_ref, rw, rd, perm, kq, ph, tb, acc, sb, r2,
           s3, r3, fs, w_send, w_recv, d_send, d_recv, l_sem, send2, recv2, send3, recv3):
    z = lax.axis_index("op")
    row = lax.axis_index("row")
    y, x, c = row // 8, (row // 2) % 4, row % 2
    nc = 1 - c
    along = x * nc + y * c
    across = y * nc + x * c
    slot_x = x * 2 + c
    slot_y = y * 2 + c

    def dev(yy, xx, cc):
        return yy * 8 + xx * 2 + cc

    for s in range(8):
        rd[s, pl.ds(NR_LOC, 3)] = jnp.zeros((3, 2, 8, 128), BF16)

    barrier = pltpu.get_barrier_semaphore()
    me_line = z * 8 + x * 2 + c

    def greet_y(j, carry):
        o = (me_line + j) % 32
        pl.semaphore_signal(barrier, inc=1, device_id=(o // 8, y * 8 + o % 8), device_id_type=MESH)
        return carry

    def greet_x(j, carry):
        yy = (y + 1 + j // 8) % 4
        pl.semaphore_signal(
            barrier, inc=1, device_id=((j // 2) % 4, dev(yy, x, j % 2)), device_id_type=MESH
        )
        return carry

    lax.fori_loop(1, 32, greet_y, 0)
    lax.fori_loop(0, 24, greet_x, 0)
    pl.semaphore_wait(barrier, 55)

    def word_copy(k, slot, target):
        return pltpu.make_async_remote_copy(
            src_ref=words_ref, dst_ref=rw.at[slot], send_sem=w_send.at[k],
            recv_sem=w_recv.at[slot], device_id=target, device_id_type=MESH,
        )

    def data_src(tile, h):
        start, size = HALVES[h]
        return ops_ref.at[z // 2, pl.ds(start, size), :, tile]

    def data_dst(slot, h):
        start, size = HALVES[h]
        return rd.at[slot, pl.ds(start, size)]

    def data_copy(k, slot, tile, h, target):
        return pltpu.make_async_remote_copy(
            src_ref=data_src(tile, h), dst_ref=data_dst(slot, h), send_sem=d_send.at[k, h],
            recv_sem=d_recv.at[slot, h], device_id=target, device_id_type=MESH,
        )

    base = (z % 2) * 8
    peers = []
    for j in (1, 3, 2):
        xx = (x + j) % 4
        yy = (y + j) % 4
        peers.append((slot_x, base + xx, (z, dev(y, xx, 0))))
        peers.append((slot_y, base + 4 + yy, (z, dev(yy, x, 1))))
    partner_slot = slot_x * c + slot_y * nc
    partner_tile = base + nc * 4 + x * c + y * nc
    peers.append((partner_slot, partner_tile, (z, dev(y, x, nc))))
    own_slot = along * 2 + c
    own_tile = base + c * 4 + along

    for k, (slot, tile, target) in enumerate(peers):
        word_copy(k, slot, target).start()
    order = [(0, 0), (1, 0), (2, 0), (3, 0), (6, 0), (0, 1), (1, 1), (2, 1), (3, 1), (6, 1),
             (4, 0), (5, 0), (4, 1), (5, 1)]
    for k, h in order:
        slot, tile, target = peers[k]
        data_copy(k, slot, tile, h, target).start()
    for h in range(2):
        pltpu.make_async_copy(data_src(own_tile, h), data_dst(own_slot, h), l_sem.at[h]).start()
    own_words = pltpu.make_async_copy(words_ref, rw.at[own_slot], l_sem.at[2])
    own_words.start()

    o_i = lax.broadcasted_iota(jnp.int32, (256, 256), 0)
    i_i = lax.broadcasted_iota(jnp.int32, (256, 256), 1)
    perm[...] = jnp.where(i_i == (o_i % 32) * 8 + o_i // 32, 1.0, 0.0).astype(BF16)

    m_i = lax.broadcasted_iota(jnp.int32, (1024, 256), 0)
    g_i, o32 = m_i // 256, (m_i // 8) % 32
    zc = (o32 // 8) * 32 + o32 % 2
    a_i = (o32 // 2) % 4
    owner = zc + (g_i * 8 + a_i * 2) * nc + (a_i * 8 + g_i * 2) * c
    k_i = owner * 2 + (m_i // 4) % 2
    pick = jnp.where(lax.broadcasted_iota(jnp.int32, (1024, 256), 1) == k_i, 1.0, 0.0).astype(BF16)
    kxyz = mm(pick, kp_ref[...])
    m_l = lax.broadcasted_iota(jnp.int32, (1024, 128), 0)
    lane = lax.broadcasted_iota(jnp.int32, (1024, 128), 1)
    turns = (4 * (((m_l // 2) % 2 + 3 * (m_l % 2)) % 4)).astype(F32)
    kq[...] = jnp.where(lane < 3, kxyz, jnp.where(lane == 3, turns, jnp.where(lane == 4, 1.0, 0.0))).astype(BF16)

    own_words.wait()
    for slot in range(8):
        @pl.when(slot != own_slot)
        def _():
            word_copy(0, slot, (z, row)).wait_recv()

    r_row = lax.broadcasted_iota(jnp.int32, (128, 128), 0)
    r_lane = lax.broadcasted_iota(jnp.int32, (128, 128), 1)
    comp_row = (lax.broadcasted_iota(jnp.int32, (256, 128), 0) // 2) % 2 == 1
    quarter = jnp.where(r_lane >= 64, 4.0, 0.0)

    def phases(i, carry):
        slot, h = i // 2, i % 2
        word = rw[slot, pl.ds(h, 1)]
        rx = (word % 32 - 8).astype(F32)
        ry = ((word // 32) % 32 - 8).astype(F32)
        rz = ((word // 1024) % 32 - 8).astype(F32)
        deg = (word // 32768).astype(F32)
        weight = jnp.where(deg > 0.0, 1.0 / jnp.maximum(deg, 1.0), 0.0)
        along_x = rx * 0.125
        rmat = jnp.where(r_row == 0, rx, jnp.where(r_row == 1, ry, jnp.where(r_row == 2, rz, jnp.where(
            r_row == 3, 1.0, jnp.where(r_row == 4, quarter, 0.0))))).astype(BF16)
        step = (slot // 2) * 2 + h
        col = pl.multiple_of((slot % 2) * 128, 128)

        def block(b, cc):
            rows = pl.ds(pl.multiple_of(b * 256, 256), 256)
            u = mm(kq[rows, :], rmat)
            u = u - 16.0 * jnp.floor(u * 0.0625)
            t = jnp.abs(u - 8.0) - 4.0
            s = t * t
            v = t * (S0 + s * (S1 + s * (S2 + s * S3))) * weight
            v = jnp.where(comp_row, v * along_x, v)
            ph[step, rows, pl.ds(col, 128)] = v.astype(BF16)
            return cc

        lax.fori_loop(0, 4, block, 0)
        return carry

    lax.fori_loop(0, 16, phases, 0)

    def wait_data(chip, h):
        for cc in range(2):
            slot = chip * 2 + cc

            @pl.when(slot == own_slot)
            def _():
                pltpu.make_async_copy(data_src(own_tile, h), data_dst(slot, h), l_sem.at[h]).wait()

            @pl.when(slot != own_slot)
            def _():
                data_copy(0, slot, own_tile, h, (z, row)).wait_recv()

    def regroup(chip, h):
        for cc in range(2):
            for q in range(2):
                at = pl.ds(h * 64 + q * 32, 32)
                both = jnp.concatenate(
                    [rd[chip * 2 + cc, at, p].reshape(256, 128) for p in range(2)], axis=1
                )
                out = mm(perm[...], both).astype(BF16)
                for p in range(2):
                    for r in range(8):
                        tb[pl.ds(cc * 128 + p * 64 + q * 32, 32), pl.ds(r * 128, 128)] = out[
                            r * 32:(r + 1) * 32, p * 128:(p + 1) * 128
                        ]

    steps = [(0, 0), (0, 1), (1, 0), (3, 0), (1, 1), (3, 1), (2, 0), (2, 1)]
    for n, (off, h) in enumerate(steps[:-1]):
        chip = (along + off) % 4
        wait_data(chip, h)
        regroup(chip, h)

        def add(b, carry):
            rows = pl.ds(pl.multiple_of(b * 256, 256), 256)
            term = mm(ph[chip * 2 + h, rows, :], tb[...])
            if n == 0:
                acc[rows, :] = term
            else:
                acc[rows, :] = acc[rows, :] + term
            return carry

        lax.fori_loop(0, 4, add, 0)

    off, h = steps[-1]
    chip = (along + off) % 4
    wait_data(chip, h)
    regroup(chip, h)

    def partial_copy(g):
        yy, xx = g * nc + y * c, x * nc + g * c
        return pltpu.make_async_remote_copy(
            src_ref=sb.at[g], dst_ref=r2.at[across], send_sem=send2.at[g],
            recv_sem=recv2.at[across], device_id=(z, dev(yy, xx, c)), device_id_type=MESH,
        )

    def partial_from(g):
        return pltpu.make_async_remote_copy(
            src_ref=sb.at[g], dst_ref=r2.at[g], send_sem=send2.at[g],
            recv_sem=recv2.at[g], device_id=(z, row), device_id_type=MESH,
        )

    groups = [(across + j) % 4 for j in (2, 1, 3, 0)]
    for n, g in enumerate(groups):
        rows = pl.ds(pl.multiple_of(g * 256, 256), 256)
        term = acc[rows, :] + mm(ph[chip * 2 + h, rows, :], tb[...])
        if n < 3:
            sb[g] = term.astype(BF16)
        else:
            acc[rows, :] = term
        if n > 0:
            partial_copy(groups[n - 1]).start()

    for n in (1, 2, 0):
        partial_from(groups[n]).wait_recv()

    def owner_copy(o, slot):
        zz, aa, cc = o // 8, (o // 2) % 4, o % 2
        yy, xx = y * nc + aa * c, aa * nc + x * c
        return pltpu.make_async_remote_copy(
            src_ref=s3.at[o], dst_ref=r3.at[slot], send_sem=send3.at[o],
            recv_sem=recv3.at[slot], device_id=(zz, dev(yy, xx, cc)), device_id_type=MESH,
        )

    me_o = z * 8 + along * 2 + c
    my_slot = z * 8 + c * 4 + along

    def finish(b):
        rows = pl.ds(pl.multiple_of(across * 256 + b * 64, 64), 64)
        part = pl.ds(pl.multiple_of(b * 64, 64), 64)
        total = acc[rows, :]
        for n in range(3):
            total = total + r2[groups[n], part, :].astype(F32)
        s3[pl.ds(b * 8, 8)] = total.reshape(8, 8, 1024).astype(BF16)

    def send_block(b):
        def one(i, carry):
            o = b * 8 + i

            @pl.when(o != me_o)
            def _():
                owner_copy(o, my_slot).start()
            return carry

        lax.fori_loop(0, 8, one, 0)

    blocks = [(z + j) % 4 for j in (2, 1, 3, 0)]
    for n, b in enumerate(blocks):
        finish(b)
        if n > 0:
            send_block(blocks[n - 1])
    send_block(blocks[3])
    own3 = pltpu.make_async_copy(s3.at[me_o], r3.at[my_slot], l_sem.at[3])
    own3.start()
    own3.wait()

    def collect(slot, carry):
        @pl.when(slot != my_slot)
        def _():
            owner_copy(slot, slot).wait_recv()

        op, t = slot // 16, slot % 16
        for r in range(8):
            fs[pl.ds(op * 1024 + t * 8 + r, 8, stride=128), :] = r3[slot, :, r * 128:(r + 1) * 128].astype(F32)
        return carry

    lax.fori_loop(0, 32, collect, 0)

    for k2 in range(2):
        vs = v_ref[k2].reshape(128, 128)
        sums = []
        for j in range(4):
            for ri in range(2):
                at = ((j // 2) * 8 + k2 * 4 + (j % 2) * 2 + ri) * 128
                sums.append(fs[at:at + 128, :].astype(BF16))
        left = mm(vs, jnp.concatenate(sums, axis=1))
        parts = []
        for j in range(4):
            lr = left[:, (2 * j) * 128:(2 * j + 1) * 128]
            li = left[:, (2 * j + 1) * 128:(2 * j + 2) * 128]
            parts.append(lr[:64] + li[64:])
            parts.append(li[:64] - lr[64:])
        stack = jnp.concatenate(parts, axis=0)
        high = stack.astype(BF16)
        low = (stack - high.astype(F32)).astype(BF16)
        vr, vi = v_ref[k2, 0], v_ref[k2, 1]
        yr = nt(high, vr) + nt(low, vr)
        yi = nt(high, vi) + nt(low, vi)
        res = []
        for j in range(4):
            a, b = slice(128 * j, 128 * j + 64), slice(128 * j + 64, 128 * j + 128)
            res.append((yr[a] - yi[b], yi[a] + yr[b]))
        (hr, hi), (dr, di), (ar, ai), (er, ei) = res
        qr, qi = hr - di, hi + dr
        pr, pi = hr + di, hi - dr
        gr = mm(ar, qr, HIGH) - mm(ai, qi, HIGH) + mm(pr, ar, HIGH) - mm(pi, ai, HIGH)
        gi = mm(ar, qi, HIGH) + mm(ai, qr, HIGH) + mm(pr, ai, HIGH) + mm(pi, ar, HIGH)
        out_ref[k2, 0] = er + FACTOR * gr
        out_ref[k2, 1] = ei + FACTOR * gi

    for k, (slot, tile, target) in enumerate(peers):
        word_copy(k, slot, target).wait_send()
        for h in range(2):
            data_copy(k, slot, tile, h, target).wait_send()
    for g in groups[:3]:
        partial_copy(g).wait_send()

    def drain(o, carry):
        @pl.when(o != me_o)
        def _():
            owner_copy(o, my_slot).wait_send()
        return carry

    lax.fori_loop(0, 32, drain, 0)


def on_device(wannier_ops, r_coords, degeneracy, kpoints, bloch_vectors):
    ops = wannier_ops.reshape(2, NR_LOC, 2, 16, 8, 128)
    shifted = r_coords + 8
    word = shifted[:, 0] + shifted[:, 1] * 32 + shifted[:, 2] * 1024 + degeneracy * 32768
    word = jnp.pad(word, (0, 128 - NR_LOC)).reshape(2, 64)
    words = jnp.concatenate([word, word], axis=1)
    kp = jnp.pad(kpoints, ((0, 0), (0, 125))).astype(BF16)
    dma = pltpu.SemaphoreType.DMA
    res = pl.pallas_call(
        kernel,
        out_shape=jax.ShapeDtypeStruct((2, 2, BANDS, BANDS), F32),
        in_specs=[pl.BlockSpec(memory_space=pltpu.VMEM)] * 3 + [pl.BlockSpec(memory_space=pl.ANY)],
        out_specs=pl.BlockSpec(memory_space=pltpu.VMEM),
        scratch_shapes=[
            pltpu.VMEM((8, 2, 128), jnp.int32),
            pltpu.VMEM((8, 128, 2, 8, 128), BF16),
            pltpu.VMEM((256, 256), BF16),
            pltpu.VMEM((1024, 128), BF16),
            pltpu.VMEM((8, 1024, 256), BF16),
            pltpu.VMEM((256, 1024), BF16),
            pltpu.VMEM((1024, 1024), F32),
            pltpu.VMEM((4, 256, 1024), BF16),
            pltpu.VMEM((4, 256, 1024), BF16),
            pltpu.VMEM((32, 8, 1024), BF16),
            pltpu.VMEM((32, 8, 1024), BF16),
            pltpu.VMEM((2048, 128), F32),
            dma((7,)), dma((8,)), dma((7, 2)), dma((8, 2)), dma((4,)),
            dma((4,)), dma((4,)), dma((32,)), dma((32,)),
        ],
        compiler_params=pltpu.CompilerParams(
            collective_id=0, has_side_effects=True, vmem_limit_bytes=48 * 1024 * 1024
        ),
    )(words, kp, bloch_vectors, ops)
    return res.reshape(2, 2, BANDS * BANDS)


def solution(mesh):
    in_specs = (
        P(None, "row", None, None, None),
        P("row", None),
        P("row"),
        P(),
        P(("op", "row"), None, None, None),
    )
    return jax.shard_map(
        on_device, mesh=mesh, in_specs=in_specs, out_specs=P(("op", "row"), None, None), check_vma=False
    )
```

```python
import jax
import jax.numpy as jnp
from jax import lax
from jax.experimental import pallas as pl
from jax.experimental.pallas import tpu as pltpu
from jax.sharding import PartitionSpec as P

MESH = pl.DeviceIdType.MESH
HIGH = lax.Precision.HIGHEST
F32 = jnp.float32
BF16 = jnp.bfloat16
I32 = jnp.int32

NR_LOC = 125
SIZES = (64, 61)
PASSES = 2
ROWS = 8 // PASSES
WIDE = ROWS * 128
GROUP = 256 // ROWS
BANDS = 64
FACTOR = 1.0 / 8.0
S0 = 0.392698743691337 * 16.0
S1 = -0.010092707352671412 * 16.0 ** 3
S2 = 7.766394538597307e-05 * 16.0 ** 5
S3 = -2.6791896176843414e-07 * 16.0 ** 7
MAGIC = 12582912.0


def nt(a, b, precision=None):
    return lax.dot_general(
        a, b, (((1,), (1,)), ((), ())), preferred_element_type=F32, precision=precision
    )


def mm(a, b, precision=None):
    return jnp.dot(a, b, preferred_element_type=F32, precision=precision)


def iota(shape, dim):
    return lax.broadcasted_iota(I32, shape, dim)


def kernel(coord_ref, deg_ref, kp_ref, v_ref, ops_ref, out_ref, rc, rg, rd, kps, vs_ref, perm, pick,
           kpp, kq, cm, wx, rmat, ph, tb, acc, sb, r2, s3, r3, fs, c_send, c_recv, g_send, g_recv,
           d_send, d_recv, l_sem, send2, recv2, send3, recv3):
    z = lax.axis_index("op")
    row = lax.axis_index("row")
    y, x, c = row // 8, (row // 2) % 4, row % 2
    nc = 1 - c
    along = x * nc + y * c
    across = y * nc + x * c
    slot_x = x * 2 + c
    slot_y = y * 2 + c

    def dev(yy, xx, cc):
        return yy * 8 + xx * 2 + cc

    for p in range(PASSES):
        for s in range(8):
            rd[p, s, pl.ds(NR_LOC, 3)] = jnp.zeros((3, 2, ROWS, 128), BF16)

    barrier = pltpu.get_barrier_semaphore()

    def greet(zz, rr):
        pl.semaphore_signal(barrier, inc=1, device_id=(zz, rr), device_id_type=MESH)

    for j in (2, 1, 3):
        yy, xx, zz = (y + j) % 4, (x + j) % 4, (z + j) % 4
        near = dev(y * nc + yy * c, xx * nc + x * c, 0)
        greet(z, near)
        greet(z, near + 1)
        greet(z, dev(yy * nc + y * c, x * nc + xx * c, c))
        greet(zz, row)
    greet(z, dev(y, x, nc))

    base = (z % 2) * 8

    def data_src(tile, p, h):
        return ops_ref.at[z // 2, pl.ds(64 * h, SIZES[h]), :, tile, p]

    def data_dst(slot, p, h):
        return rd.at[p, slot, pl.ds(64 * h, SIZES[h])]

    def data_copy(k, slot, tile, p, h, target):
        return pltpu.make_async_remote_copy(
            src_ref=data_src(tile, p, h), dst_ref=data_dst(slot, p, h), send_sem=d_send.at[k, p, h],
            recv_sem=d_recv.at[slot, p, h], device_id=target, device_id_type=MESH,
        )

    own_slot = along * 2 + c
    own_tile = base + c * 4 + along

    def own_data(p, h):
        return pltpu.make_async_copy(
            data_src(own_tile, p, h), data_dst(own_slot, p, h), d_recv.at[own_slot, p, h]
        )

    kp_copy = pltpu.make_async_copy(kp_ref, kps, l_sem.at[0])
    v_copy = pltpu.make_async_copy(v_ref, vs_ref, l_sem.at[1])
    own_coord = pltpu.make_async_copy(coord_ref, rc.at[own_slot], c_recv.at[own_slot])
    own_deg = pltpu.make_async_copy(deg_ref, rg.at[own_slot], g_recv.at[own_slot])
    for copy in (kp_copy, own_coord, own_deg, v_copy):
        copy.start()
    for p in range(PASSES):
        for h in range(2):
            own_data(p, h).start()

    m_i = iota((1024, 128), 0)
    lane = iota((1024, 128), 1)
    g_i, o32 = m_i // 256, (m_i // 8) % 32
    a_i = (o32 // 2) % 4
    owner = (o32 // 8) * 32 + o32 % 2 + (g_i * 8 + a_i * 2) * nc + (a_i * 8 + g_i * 2) * c
    k_i = owner * 2 + (m_i // 4) % 2
    for half in range(2):
        pick[:, half * 128:(half + 1) * 128] = jnp.where(lane + 128 * half == k_i, 1.0, 0.0).astype(BF16)

    peers = []
    for j in (1, 3, 2):
        xx = (x + j) % 4
        yy = (y + j) % 4
        peers.append((slot_x, base + xx, (z, dev(y, xx, 0))))
        peers.append((slot_y, base + 4 + yy, (z, dev(yy, x, 1))))
    peers.append((slot_x * c + slot_y * nc, base + nc * 4 + x * c + y * nc, (z, dev(y, x, nc))))

    def coord_copy(k, slot, target):
        return pltpu.make_async_remote_copy(
            src_ref=coord_ref, dst_ref=rc.at[slot], send_sem=c_send.at[k],
            recv_sem=c_recv.at[slot], device_id=target, device_id_type=MESH,
        )

    def deg_copy(k, slot, target):
        return pltpu.make_async_remote_copy(
            src_ref=deg_ref, dst_ref=rg.at[slot], send_sem=g_send.at[k],
            recv_sem=g_recv.at[slot], device_id=target, device_id_type=MESH,
        )

    pl.semaphore_wait(barrier, 13)
    for k, (slot, tile, target) in enumerate(peers):
        coord_copy(k, slot, target).start()
        deg_copy(k, slot, target).start()
    order = [(0, 0), (1, 0), (2, 0), (3, 0), (6, 0), (0, 1), (1, 1), (2, 1), (3, 1), (6, 1),
             (4, 0), (5, 0), (4, 1), (5, 1)]
    for p in range(PASSES):
        for k, h in order:
            slot, tile, target = peers[k]
            data_copy(k, slot, tile, p, h, target).start()

    o_i, i_i = iota((256, 256), 0), iota((256, 256), 1)
    perm[...] = jnp.where(i_i == (o_i % GROUP) * ROWS + o_i // GROUP, 1.0, 0.0).astype(BF16)

    kpp[...] = jnp.zeros(kpp.shape, F32)
    kp_copy.wait()
    kpp[0:3, :] = kps[...].astype(F32)
    kxyz = nt(pick[...], kpp[...].astype(BF16))
    turns = (((m_i // 2) % 2 + 3 * (m_i % 2)) % 4).astype(F32) * 0.25
    kq[...] = jnp.where(lane < 3, kxyz, jnp.where(lane == 3, turns, jnp.where(lane == 4, 1.0, 0.0))).astype(BF16)

    cm[...] = jnp.zeros(cm.shape, F32)
    rmat[...] = jnp.zeros(rmat.shape, BF16)
    own_coord.wait()
    own_deg.wait()
    for slot in range(8):
        @pl.when(slot != own_slot)
        def _():
            coord_copy(0, slot, (z, row)).wait_recv()
            deg_copy(0, slot, (z, row)).wait_recv()

        cm[slot * 8:slot * 8 + 3, 0:NR_LOC] = rc[slot].astype(F32)
        cm[slot * 8 + 3:slot * 8 + 4, 0:NR_LOC] = rg[slot].astype(F32)
    s_r, s_l = iota((128, 256), 0), iota((128, 256), 1)
    spread = jnp.where(s_r == (s_l // 128) * 64 + s_l % 64, 1.0, 0.0).astype(BF16)
    wx[...] = mm(cm[...].astype(BF16), spread)

    row8, lane8 = iota((8, 128), 0), iota((8, 128), 1)
    quarter = jnp.where(lane8 >= 64, 0.25, 0.0)

    def phases(i, carry):
        chip, h = i // 2, i % 2
        amps = []
        for cc in range(2):
            blk = wx[pl.ds(pl.multiple_of((chip * 2 + cc) * 8, 8), 8), pl.ds(pl.multiple_of(h * 128, 128), 128)]
            deg = blk[3:4]
            weight = jnp.where(deg > 0.0, 1.0 / jnp.maximum(deg, 1.0), 0.0)
            moment = weight * (blk[0:1] * 0.125)
            amps.append(jnp.where((row8 // 2) % 2 == 1, moment, weight))
            top = jnp.where(row8 < 3, blk * 0.0625, jnp.where(row8 == 3, 1.0, jnp.where(row8 == 4, quarter, 0.0)))
            rmat[0:16, cc * 128:(cc + 1) * 128] = jnp.concatenate([top, jnp.zeros((8, 128), F32)], axis=0).astype(BF16)
        amp = jnp.concatenate(amps, axis=1)

        def block(b, cc):
            rows = pl.ds(pl.multiple_of(b * 256, 256), 256)
            u = mm(kq[rows, :], rmat[...])
            u = u - ((u + MAGIC) - MAGIC)
            t = 0.25 - jnp.abs(u)
            s = t * t
            v = t * (S0 + s * (S1 + s * (S2 + s * S3)))
            v = (v.reshape(32, 8, 256) * amp[None]).reshape(256, 256)
            ph[i, rows, :] = v.astype(BF16)
            return cc

        lax.fori_loop(0, 4, block, 0)
        return carry

    lax.fori_loop(0, 8, phases, 0)

    def gather(p, i):
        off = jnp.where(i < 2, 0, jnp.where(i >= 6, 2, 1 + 2 * (i % 2)))
        h = jnp.where(i < 2, i, jnp.where(i < 4, 0, jnp.where(i < 6, 1, i - 6)))
        chip = (along + off) % 4
        for cc in range(2):
            slot = chip * 2 + cc
            for hh in range(2):
                @pl.when(h == hh)
                def _():
                    @pl.when(slot == own_slot)
                    def _():
                        own_data(p, hh).wait()

                    @pl.when(slot != own_slot)
                    def _():
                        data_copy(0, slot, own_tile, p, hh, (z, row)).wait_recv()

            for q in range(64 // GROUP):
                at = pl.ds(h * 64 + q * GROUP, GROUP)
                both = jnp.concatenate(
                    [rd[p, slot, at, part].reshape(256, 128) for part in range(2)], axis=1
                )
                out = mm(perm[...], both).astype(BF16)
                for part in range(2):
                    for r in range(ROWS):
                        tb[pl.ds(cc * 128 + part * 64 + q * GROUP, GROUP), pl.ds(r * 128, 128)] = out[
                            r * GROUP:(r + 1) * GROUP, part * 128:(part + 1) * 128
                        ]
        return chip * 2 + h

    def partial_copy(p, g):
        yy, xx = g * nc + y * c, x * nc + g * c
        return pltpu.make_async_remote_copy(
            src_ref=sb.at[p, g], dst_ref=r2.at[p, across], send_sem=send2.at[p, g],
            recv_sem=recv2.at[p, across], device_id=(z, dev(yy, xx, c)), device_id_type=MESH,
        )

    def partial_from(p, g):
        return pltpu.make_async_remote_copy(
            src_ref=sb.at[p, g], dst_ref=r2.at[p, g], send_sem=send2.at[p, g],
            recv_sem=recv2.at[p, g], device_id=(z, row), device_id_type=MESH,
        )

    groups = [(across + j) % 4 for j in (2, 1, 3)]

    for p in range(PASSES):
        acc[p] = jnp.zeros(acc.shape[1:], F32)

        def step(i, carry):
            at = gather(p, i)
            for n in range(WIDE // 256):
                cols = slice(n * 256, (n + 1) * 256)
                acc[p, :, cols] = acc[p, :, cols] + mm(ph[at], tb[:, cols])
            return carry

        lax.fori_loop(0, 7, step, 0)
        at = gather(p, 7)
        for n in range(WIDE // 256):
            cols = slice(n * 256, (n + 1) * 256)
            full = acc[p, :, cols] + mm(ph[at], tb[:, cols])
            acc[p, :, cols] = full
            sb[p, :, :, cols] = full.reshape(4, 256, 256).astype(BF16)
        for g in groups:
            partial_copy(p, g).start()

    def owner_copy(p, o, slot):
        zz, aa, cc = o // 8, (o // 2) % 4, o % 2
        yy, xx = y * nc + aa * c, aa * nc + x * c
        return pltpu.make_async_remote_copy(
            src_ref=s3.at[p, o], dst_ref=r3.at[p, slot], send_sem=send3.at[p, o],
            recv_sem=recv3.at[p, slot], device_id=(zz, dev(yy, xx, cc)), device_id_type=MESH,
        )

    me_o = z * 8 + along * 2 + c
    my_slot = z * 8 + c * 4 + along

    def own_sum(p):
        return pltpu.make_async_copy(s3.at[p, me_o], r3.at[p, my_slot], recv3.at[p, my_slot])

    def finish(p, b):
        rows = pl.ds(pl.multiple_of(across * 256 + b * 64, 64), 64)
        part = pl.ds(pl.multiple_of(b * 64, 64), 64)
        total = acc[p, rows, :]
        for g in groups:
            total = total + r2[p, g, part, :].astype(F32)
        s3[p, pl.ds(b * 8, 8)] = total.reshape(8, 8, WIDE).astype(BF16)

    def send_block(p, b):
        def one(i, carry):
            o = b * 8 + i

            @pl.when(o != me_o)
            def _():
                owner_copy(p, o, my_slot).start()
            return carry

        lax.fori_loop(0, 8, one, 0)

    blocks = [(z + j) % 4 for j in (2, 1, 3, 0)]
    for p in range(PASSES):
        for g in (groups[1], groups[2], groups[0]):
            partial_from(p, g).wait_recv()
        for n, b in enumerate(blocks):
            finish(p, b)
            if n > 0:
                send_block(p, blocks[n - 1])
        send_block(p, blocks[3])
        own_sum(p).start()

    for p in range(PASSES):
        own_sum(p).wait()

        def collect(slot, carry):
            @pl.when(slot != my_slot)
            def _():
                owner_copy(p, slot, slot).wait_recv()

            op, t = slot // 16, slot % 16
            for r in range(ROWS):
                fs[pl.ds(op * 1024 + t * 8 + p * ROWS + r, 8, stride=128), :] = r3[
                    p, slot, :, r * 128:(r + 1) * 128
                ].astype(F32)
            return carry

        lax.fori_loop(0, 32, collect, 0)

    v_copy.wait()
    for k2 in range(2):
        vs = vs_ref[k2].reshape(128, 128)
        sums = []
        for j in range(4):
            for ri in range(2):
                at = ((j // 2) * 8 + k2 * 4 + (j % 2) * 2 + ri) * 128
                sums.append(fs[at:at + 128, :].astype(BF16))
        left = mm(vs, jnp.concatenate(sums, axis=1))
        parts = []
        for j in range(4):
            lr = left[:, (2 * j) * 128:(2 * j + 1) * 128]
            li = left[:, (2 * j + 1) * 128:(2 * j + 2) * 128]
            parts.append(lr[:64] + li[64:])
            parts.append(li[:64] - lr[64:])
        stack = jnp.concatenate(parts, axis=0)
        high = stack.astype(BF16)
        low = (stack - high.astype(F32)).astype(BF16)
        vr, vi = vs_ref[k2, 0], vs_ref[k2, 1]
        yr = nt(high, vr) + nt(low, vr)
        yi = nt(high, vi) + nt(low, vi)
        res = []
        for j in range(4):
            a, b = slice(128 * j, 128 * j + 64), slice(128 * j + 64, 128 * j + 128)
            res.append((yr[a] - yi[b], yi[a] + yr[b]))
        (hr, hi), (dr, di), (ar, ai), (er, ei) = res
        qr, qi = hr - di, hi + dr
        pr, pi = hr + di, hi - dr
        gr = mm(ar, qr, HIGH) - mm(ai, qi, HIGH) + mm(pr, ar, HIGH) - mm(pi, ai, HIGH)
        gi = mm(ar, qi, HIGH) + mm(ai, qr, HIGH) + mm(pr, ai, HIGH) + mm(pi, ar, HIGH)
        out_ref[k2, 0] = er + FACTOR * gr
        out_ref[k2, 1] = ei + FACTOR * gi

    for k, (slot, tile, target) in enumerate(peers):
        coord_copy(k, slot, target).wait_send()
        deg_copy(k, slot, target).wait_send()
        for p in range(PASSES):
            for h in range(2):
                data_copy(k, slot, tile, p, h, target).wait_send()
    for p in range(PASSES):
        for g in groups:
            partial_copy(p, g).wait_send()

        def drain(o, carry):
            @pl.when(o != me_o)
            def _():
                owner_copy(p, o, my_slot).wait_send()
            return carry

        lax.fori_loop(0, 32, drain, 0)


def on_device(wannier_ops, r_coords, degeneracy, kpoints, bloch_vectors):
    ops = wannier_ops.reshape(2, NR_LOC, 2, 16, PASSES, ROWS, 128)
    dma = pltpu.SemaphoreType.DMA
    vmem = pltpu.VMEM
    res = pl.pallas_call(
        kernel,
        out_shape=jax.ShapeDtypeStruct((2, 2, BANDS, BANDS), F32),
        in_specs=[pl.BlockSpec(memory_space=pl.ANY)] * 5,
        out_specs=pl.BlockSpec(memory_space=vmem),
        scratch_shapes=[
            vmem((8, 3, NR_LOC), I32),
            vmem((8, 1, NR_LOC), I32),
            vmem((PASSES, 8, 128, 2, ROWS, 128), BF16),
            vmem((3, 256), I32),
            vmem((2, 2, 64, 128), BF16),
            vmem((256, 256), BF16),
            vmem((1024, 256), BF16),
            vmem((128, 256), F32),
            vmem((1024, 128), BF16),
            vmem((64, 128), F32),
            vmem((64, 256), F32),
            vmem((128, 256), BF16),
            vmem((8, 1024, 256), BF16),
            vmem((256, WIDE), BF16),
            vmem((PASSES, 1024, WIDE), F32),
            vmem((PASSES, 4, 256, WIDE), BF16),
            vmem((PASSES, 4, 256, WIDE), BF16),
            vmem((PASSES, 32, 8, WIDE), BF16),
            vmem((PASSES, 32, 8, WIDE), BF16),
            vmem((2048, 128), F32),
            dma((7,)), dma((8,)), dma((7,)), dma((8,)), dma((7, PASSES, 2)), dma((8, PASSES, 2)), dma((2,)),
            dma((PASSES, 4)), dma((PASSES, 4)), dma((PASSES, 32)), dma((PASSES, 32)),
        ],
        compiler_params=pltpu.CompilerParams(
            collective_id=0, has_side_effects=True, vmem_limit_bytes=56 * 1024 * 1024
        ),
    )(r_coords.T, degeneracy.reshape(1, NR_LOC), kpoints.T, bloch_vectors, ops)
    return res.reshape(2, 2, BANDS * BANDS)


def solution(mesh):
    in_specs = (
        P(None, "row", None, None, None),
        P("row", None),
        P("row"),
        P(),
        P(("op", "row"), None, None, None),
    )
    return jax.shard_map(
        on_device, mesh=mesh, in_specs=in_specs, out_specs=P(("op", "row"), None, None), check_vma=False
    )
```

```python
import jax
import jax.numpy as jnp
from jax import lax
from jax.experimental import pallas as pl
from jax.experimental.pallas import tpu as pltpu
from jax.sharding import PartitionSpec as P

MESH = pl.DeviceIdType.MESH
HIGH = lax.Precision.HIGHEST
F32 = jnp.float32
BF16 = jnp.bfloat16
I32 = jnp.int32

NR_LOC = 125
SIZES = (64, 61)
PASSES = 4
ROWS = 8 // PASSES
WIDE = ROWS * 128
TILES = WIDE // 256
SUB = 256
PER = WIDE // SUB
SUBS = PASSES * PER
LAG = 2 if SUBS > 2 else 1
TALL = 64 * ROWS
FACTOR = 1.0 / 8.0
S0 = 0.392698743691337 * 16.0
S1 = -0.010092707352671412 * 16.0 ** 3
S2 = 7.766394538597307e-05 * 16.0 ** 5
S3 = -2.6791896176843414e-07 * 16.0 ** 7
MAGIC = 12582912.0


def nt(a, b, precision=None):
    return lax.dot_general(
        a, b, (((1,), (1,)), ((), ())), preferred_element_type=F32, precision=precision
    )


def mm(a, b, precision=None):
    return jnp.dot(a, b, preferred_element_type=F32, precision=precision)


def iota(shape, dim):
    return lax.broadcasted_iota(I32, shape, dim)


def kernel(coord_ref, deg_ref, kp_ref, v_ref, ops_ref, out_ref, rc, rg, rd, kps, vs_ref, perm, pick,
           kpp, kq, cm, wx, rmat, tw, ph, tb, acc, sb, r2, s3, r3, fs, g, og, c_send, c_recv, g_send, g_recv,
           d_send, d_recv, l_sem, send2, recv2, send3, recv3):
    z = lax.axis_index("op")
    row = lax.axis_index("row")
    y, x, c = row // 8, (row // 2) % 4, row % 2
    nc = 1 - c
    along = x * nc + y * c
    across = y * nc + x * c
    slot_x = x * 2 + c
    slot_y = y * 2 + c

    def dev(yy, xx, cc):
        return yy * 8 + xx * 2 + cc

    def bytes_of(ref, sem):
        pltpu.make_async_copy(ref, ref, sem).wait()

    for p in range(PASSES):
        for s in range(8):
            rd[p, s, pl.ds(NR_LOC, 3)] = jnp.zeros((3, 2, ROWS, 128), BF16)

    barrier = pltpu.get_barrier_semaphore()

    def greet(zz, rr):
        pl.semaphore_signal(barrier, inc=1, device_id=(zz, rr), device_id_type=MESH)

    for j in (2, 1, 3):
        yy, xx, zz = (y + j) % 4, (x + j) % 4, (z + j) % 4
        near = dev(y * nc + yy * c, xx * nc + x * c, 0)
        greet(z, near)
        greet(z, near + 1)
        greet(z, dev(yy * nc + y * c, x * nc + xx * c, c))
        greet(zz, row)
    greet(z, dev(y, x, nc))

    base = (z % 2) * 8

    def data_src(tile, p, h):
        return ops_ref.at[z // 2, pl.ds(64 * h, SIZES[h]), :, tile, p]

    def data_dst(slot, p, h):
        return rd.at[p, slot, pl.ds(64 * h, SIZES[h])]

    def data_copy(slot, tile, p, h, target):
        return pltpu.make_async_remote_copy(
            src_ref=data_src(tile, p, h), dst_ref=data_dst(slot, p, h), send_sem=d_send,
            recv_sem=d_recv.at[slot // 2, p, h], device_id=target, device_id_type=MESH,
        )

    own_slot = along * 2 + c
    own_tile = base + c * 4 + along

    def own_data(p, h):
        return pltpu.make_async_copy(
            data_src(own_tile, p, h), data_dst(own_slot, p, h), d_recv.at[along, p, h]
        )

    kp_copy = pltpu.make_async_copy(kp_ref, kps, l_sem.at[0])
    v_copy = pltpu.make_async_copy(v_ref, vs_ref, l_sem.at[1])
    own_coord = pltpu.make_async_copy(coord_ref, rc.at[own_slot], c_recv)
    own_deg = pltpu.make_async_copy(deg_ref, rg.at[own_slot], g_recv)
    for copy in (kp_copy, own_coord, own_deg, v_copy):
        copy.start()
    for p in range(PASSES):
        for h in range(2):
            own_data(p, h).start()

    k_r, k_l = iota((256, 256), 0), iota((256, 256), 1)
    g_i, o32 = k_r // 64, (k_r // 2) % 32
    a_i = (o32 // 2) % 4
    owner = (o32 // 8) * 32 + o32 % 2 + (g_i * 8 + a_i * 2) * nc + (a_i * 8 + g_i * 2) * c
    pick[...] = jnp.where(k_l == owner * 2 + k_r % 2, 1.0, 0.0).astype(BF16)

    peers = []
    for j in (1, 3, 2):
        xx = (x + j) % 4
        yy = (y + j) % 4
        peers.append((slot_x, base + xx, (z, dev(y, xx, 0))))
        peers.append((slot_y, base + 4 + yy, (z, dev(yy, x, 1))))
    peers.append((slot_x * c + slot_y * nc, base + nc * 4 + x * c + y * nc, (z, dev(y, x, nc))))

    def coord_copy(slot, target):
        return pltpu.make_async_remote_copy(
            src_ref=coord_ref, dst_ref=rc.at[slot], send_sem=c_send,
            recv_sem=c_recv, device_id=target, device_id_type=MESH,
        )

    def deg_copy(slot, target):
        return pltpu.make_async_remote_copy(
            src_ref=deg_ref, dst_ref=rg.at[slot], send_sem=g_send,
            recv_sem=g_recv, device_id=target, device_id_type=MESH,
        )

    pl.semaphore_wait(barrier, 13)
    for slot, tile, target in peers:
        coord_copy(slot, target).start()
        deg_copy(slot, target).start()
    order = [(0, 0), (1, 0), (2, 0), (3, 0), (6, 0), (0, 1), (1, 1), (2, 1), (3, 1), (6, 1),
             (4, 0), (5, 0), (4, 1), (5, 1)]
    for p in range(PASSES):
        for k, h in order:
            slot, tile, target = peers[k]
            data_copy(slot, tile, p, h, target).start()

    o_i, i_i = iota((256, 256), 0), iota((256, 256), 1)
    p_o, p_i = iota((TALL, TALL), 0), iota((TALL, TALL), 1)
    perm[...] = jnp.where(p_i == (p_o % 64) * ROWS + p_o // 64, 1.0, 0.0).astype(BF16)

    kpp[...] = jnp.zeros(kpp.shape, F32)
    kp_copy.wait()
    kpp[0:3, :] = kps[...].astype(F32)
    kq[...] = nt(pick[...], kpp[...].astype(BF16)).astype(BF16)

    cm[...] = jnp.zeros(cm.shape, F32)
    rmat[...] = jnp.zeros(rmat.shape, BF16)
    bytes_of(rc, c_recv)
    bytes_of(rg, g_recv)
    for slot in range(8):
        at, lanes = (slot // 2) * 8, slice((slot % 2) * 128, (slot % 2) * 128 + NR_LOC)
        cm[at:at + 3, lanes] = rc[slot].astype(F32)
        cm[at + 3:at + 4, lanes] = rg[slot].astype(F32)
    s_c, s_h, s_r = (i_i % 128) // 64, i_i // 128, i_i % 64
    spread = jnp.where(o_i == s_c * 128 + s_h * 64 + s_r, 1.0, 0.0).astype(BF16)
    wx[...] = mm(cm[...].astype(BF16), spread)

    def turn_cos(u):
        u = u - ((u + MAGIC) - MAGIC)
        t = 0.25 - jnp.abs(u)
        q = t * t
        return t * (S0 + q * (S1 + q * (S2 + q * S3)))

    def phases(i, carry):
        chip, h = i // 2, i % 2
        blk = wx[pl.ds(pl.multiple_of(chip * 8, 8), 8), pl.ds(pl.multiple_of(h * 128, 128), 128)]
        deg = blk[3:4]
        weight = jnp.where(deg > 0.0, 1.0 / jnp.maximum(deg, 1.0), 0.0)
        place = blk[0:1] * 0.125
        rmat[0:16, :] = jnp.concatenate([blk * 0.0625, jnp.zeros((8, 128), F32)], axis=0).astype(BF16)

        for b in range(4):
            u = mm(kq[b * 64:(b + 1) * 64, :], rmat[...])
            cos = turn_cos(u) * weight
            sin = turn_cos(u - 0.25) * weight
            x_cos, x_sin = cos * place, sin * place
            for q, (first, second) in enumerate(((cos, -sin), (sin, cos), (-x_sin, -x_cos), (x_cos, -x_sin))):
                at = pl.ds(b * 256 + q, 64, stride=4)
                tw[0, at, :] = first
                tw[1, at, :] = second
        for b in range(4):
            rows = slice(b * 256, (b + 1) * 256)
            for part in range(2):
                ph[i, rows, part * 128:(part + 1) * 128] = tw[part, rows, :].astype(BF16)
        return carry

    lax.fori_loop(0, 8, phases, 0)

    def gather(p, i):
        off = jnp.where(i < 2, 0, jnp.where(i >= 6, 2, 1 + 2 * (i % 2)))
        h = jnp.where(i < 2, i, jnp.where(i < 4, 0, jnp.where(i < 6, 1, i - 6)))
        chip = (along + off) % 4
        for hh in range(2):
            @pl.when(h == hh)
            def _():
                bytes_of(rd.at[p, pl.ds(0, 2), pl.ds(0, SIZES[hh])], d_recv.at[chip, p, hh])

        at = pl.ds(h * 64, 64)
        blocks = [rd[p, chip * 2 + cc, at, part].reshape(TALL, 128) for part in range(2) for cc in range(2)]
        out = mm(perm[...], jnp.concatenate(blocks, axis=1)).astype(BF16)
        for n in range(4):
            for r in range(ROWS):
                tb[n * 64:(n + 1) * 64, r * 128:(r + 1) * 128] = out[r * 64:(r + 1) * 64, n * 128:(n + 1) * 128]
        return chip * 2 + h

    def partial_copy(t, g):
        yy, xx = g * nc + y * c, x * nc + g * c
        return pltpu.make_async_remote_copy(
            src_ref=sb.at[t, g], dst_ref=r2.at[t, across], send_sem=send2.at[t],
            recv_sem=recv2.at[t], device_id=(z, dev(yy, xx, c)), device_id_type=MESH,
        )

    groups = [(across + j) % 4 for j in (2, 1, 3)]

    def send_partials(t):
        for g in groups:
            partial_copy(t, g).start()

    for p in range(PASSES):
        acc[p] = jnp.zeros(acc.shape[1:], F32)

        def step(i, carry):
            at = gather(p, i)
            for n in range(WIDE // 256):
                cols = slice(n * 256, (n + 1) * 256)
                acc[p, :, cols] = acc[p, :, cols] + mm(ph[at], tb[:, cols])
            return carry

        lax.fori_loop(0, 7, step, 0)
        at = gather(p, 7)
        for t in range(p * PER, (p + 1) * PER):
            for n in range(SUB // 256):
                here = slice(n * 256, (n + 1) * 256)
                start = (t % PER) * SUB + n * 256
                cols = slice(start, start + 256)
                full = acc[p, :, cols] + mm(ph[at], tb[:, cols])
                acc[p, :, cols] = full
                sb[t, :, :, here] = full.reshape(4, 256, 256).astype(BF16)
            send_partials(t)

    def owner_copy(t, o, zz, aa, cc):
        yy, xx = y * nc + aa * c, aa * nc + x * c
        return pltpu.make_async_remote_copy(
            src_ref=s3.at[t, o], dst_ref=r3.at[t, my_slot], send_sem=send3.at[t],
            recv_sem=recv3.at[t], device_id=(zz, dev(yy, xx, cc)), device_id_type=MESH,
        )

    me_o = z * 8 + along * 2 + c
    my_slot = z * 8 + c * 4 + along

    def finish(t, b):
        rows = pl.ds(pl.multiple_of(across * 256 + b * 64, 64), 64)
        part = pl.ds(pl.multiple_of(b * 64, 64), 64)
        n = t % PER
        total = acc[t // PER, rows, n * SUB:(n + 1) * SUB]
        for g in groups:
            total = total + r2[t, g, part, :].astype(F32)
        s3[t, pl.ds(b * 8, 8)] = total.reshape(8, 8, SUB).astype(BF16)

    def send_block(t, b):
        for i in range(8):
            aa, cc = i // 2, i % 2
            o = b * 8 + i

            @pl.when(o != me_o)
            def _():
                owner_copy(t, o, b, aa, cc).start()

    def collect(t):
        bytes_of(r3.at[t], recv3.at[t])

        def one(slot, carry):
            op, tile = slot // 16, slot % 16
            for r in range(SUB // 128):
                fs[pl.ds(op * 1024 + tile * 8 + (SUB // 128) * t + r, 8, stride=128), :] = r3[
                    t, slot, :, r * 128:(r + 1) * 128
                ].astype(F32)
            return carry

        lax.fori_loop(0, 32, one, 0)

    blocks = [(z + j) % 4 for j in (2, 1, 3, 0)]
    for t in range(SUBS):
        bytes_of(r2.at[t, pl.ds(0, 3)], recv2.at[t])
        for n, b in enumerate(blocks):
            finish(t, b)
            if n > 0:
                send_block(t, blocks[n - 1])
        send_block(t, blocks[3])
        pltpu.make_async_copy(s3.at[t, me_o], r3.at[t, my_slot], recv3.at[t]).start()
        if t >= LAG:
            collect(t - LAG)

    bytes_of(rc.at[pl.ds(0, 7)], c_send)
    bytes_of(rg.at[pl.ds(0, 7)], g_send)
    bytes_of(rd.at[:, pl.ds(0, 7), pl.ds(0, NR_LOC)], d_send)
    for t in range(SUBS):
        bytes_of(sb.at[t, pl.ds(0, 3)], send2.at[t])

    for t in range(max(SUBS - LAG, 0), SUBS):
        collect(t)

    v_copy.wait()
    for k2 in range(2):
        vs = vs_ref[k2].reshape(128, 128)
        sums = []
        for j in range(4):
            for ri in range(2):
                at = ((j // 2) * 8 + k2 * 4 + (j % 2) * 2 + ri) * 128
                sums.append(fs[at:at + 128, :].astype(BF16))
        left = mm(vs, jnp.concatenate(sums, axis=1))
        parts = []
        for j in range(4):
            lr = left[:, (2 * j) * 128:(2 * j + 1) * 128]
            li = left[:, (2 * j + 1) * 128:(2 * j + 2) * 128]
            parts.append(lr[:64] + li[64:])
            parts.append(li[:64] - lr[64:])
        stack = jnp.concatenate(parts, axis=0)
        high = stack.astype(BF16)
        low = (stack - high.astype(F32)).astype(BF16)
        vr, vi = vs_ref[k2, 0], vs_ref[k2, 1]
        yr = nt(high, vr) + nt(low, vr)
        yi = nt(high, vi) + nt(low, vi)
        res = []
        for j in range(4):
            a, b = slice(128 * j, 128 * j + 64), slice(128 * j + 64, 128 * j + 128)
            res.append((yr[a] - yi[b], yi[a] + yr[b]))
        (hr, hi), (dr, di), (ar, ai), (er, ei) = res
        qr, qi = hr - di, hi + dr
        pr, pi = hr + di, hi - dr

        def beside(*blocks):
            return jnp.concatenate(blocks, axis=1)

        first = jnp.concatenate([beside(ar, ai), beside(pr, pi)], axis=1)
        second = jnp.concatenate([beside(qr, qi), beside(-qi, qr), beside(ar, ai), beside(-ai, ar)], axis=0)
        f_high, s_high = first.astype(BF16), second.astype(BF16)
        f_low = (first - f_high.astype(F32)).astype(BF16)
        s_low = (second - s_high.astype(F32)).astype(BF16)
        both = mm(jnp.concatenate([f_high, f_low], axis=0), s_high)
        g[k2] = beside(er, ei) + FACTOR * (both[:64] + both[64:] + mm(f_high, s_low))
        even, odd = g[k2, pl.ds(0, 32, stride=2), :], g[k2, pl.ds(1, 32, stride=2), :]
        og[k2, 0] = beside(even[:, :64], odd[:, :64])
        og[k2, 1] = beside(even[:, 64:], odd[:, 64:])
        pltpu.make_async_copy(og.at[k2], out_ref.at[k2], l_sem.at[0]).start()

    for t in range(SUBS):
        bytes_of(s3.at[t, pl.ds(0, 31)], send3.at[t])
    bytes_of(og, l_sem.at[0])


def on_device(wannier_ops, r_coords, degeneracy, kpoints, bloch_vectors):
    ops = wannier_ops.reshape(2, NR_LOC, 2, 16, PASSES, ROWS, 128)
    dma = pltpu.SemaphoreType.DMA
    vmem = pltpu.VMEM
    res = pl.pallas_call(
        kernel,
        out_shape=jax.ShapeDtypeStruct((2, 2, 32, 128), F32),
        in_specs=[pl.BlockSpec(memory_space=pl.ANY)] * 5,
        out_specs=pl.BlockSpec(memory_space=pl.ANY),
        scratch_shapes=[
            vmem((8, 3, NR_LOC), I32),
            vmem((8, 1, NR_LOC), I32),
            vmem((PASSES, 8, 128, 2, ROWS, 128), BF16),
            vmem((3, 256), I32),
            vmem((2, 2, 64, 128), BF16),
            vmem((TALL, TALL), BF16),
            vmem((256, 256), BF16),
            vmem((128, 256), F32),
            vmem((256, 128), BF16),
            vmem((32, 256), F32),
            vmem((32, 256), F32),
            vmem((128, 128), BF16),
            vmem((2, 1024, 128), F32),
            vmem((8, 1024, 256), BF16),
            vmem((256, WIDE), BF16),
            vmem((PASSES, 1024, WIDE), F32),
            vmem((SUBS, 4, 256, SUB), BF16),
            vmem((SUBS, 4, 256, SUB), BF16),
            vmem((SUBS, 32, 8, SUB), BF16),
            vmem((SUBS, 32, 8, SUB), BF16),
            vmem((2048, 128), F32),
            vmem((2, 64, 128), F32),
            vmem((2, 2, 32, 128), F32),
            dma, dma, dma, dma, dma, dma((4, PASSES, 2)), dma((2,)),
            dma((SUBS,)), dma((SUBS,)), dma((SUBS,)), dma((SUBS,)),
        ],
        compiler_params=pltpu.CompilerParams(
            collective_id=0, has_side_effects=True, vmem_limit_bytes=54 * 1024 * 1024
        ),
    )(r_coords.T, degeneracy.reshape(1, NR_LOC), kpoints.T, bloch_vectors, ops)
    return res.reshape(2, 2, 4096)


def solution(mesh):
    in_specs = (
        P(None, "row", None, None, None),
        P("row", None),
        P("row"),
        P(),
        P(("op", "row"), None, None, None),
    )
    return jax.shard_map(
        on_device, mesh=mesh, in_specs=in_specs, out_specs=P(("op", "row"), None, None), check_vma=False
    )
```

```python
import jax
import jax.numpy as jnp
from jax import lax
from jax.experimental import pallas as pl
from jax.experimental.pallas import tpu as pltpu
from jax.sharding import PartitionSpec as P

MESH = pl.DeviceIdType.MESH
HIGH = lax.Precision.HIGHEST
F32 = jnp.float32
BF16 = jnp.bfloat16
I32 = jnp.int32

NR_LOC = 125
SIZES = (64, 61)
PASSES = 4
ROWS = 8 // PASSES
WIDE = ROWS * 128
TILES = WIDE // 256
SUB = 256
PER = WIDE // SUB
SUBS = PASSES * PER
LAG = 2 if SUBS > 2 else 1
TALL = 64 * ROWS
FACTOR = 1.0 / 8.0
S0 = 0.392698743691337 * 16.0
S1 = -0.010092707352671412 * 16.0 ** 3
S2 = 7.766394538597307e-05 * 16.0 ** 5
S3 = -2.6791896176843414e-07 * 16.0 ** 7
MAGIC = 12582912.0


def nt(a, b, precision=None):
    return lax.dot_general(
        a, b, (((1,), (1,)), ((), ())), preferred_element_type=F32, precision=precision
    )


def mm(a, b, precision=None):
    return jnp.dot(a, b, preferred_element_type=F32, precision=precision)


def iota(shape, dim):
    return lax.broadcasted_iota(I32, shape, dim)


def kernel(coord_ref, deg_ref, kp_ref, v_ref, ops_ref, out_ref, rc, rg, rd, kps, vs_ref, perm, pick,
           kpp, kq, cm, wx, rmat, tw, ph, tb, acc, sb, r2, s3, r3, fs, g, og, c_send, c_recv, g_send, g_recv,
           d_send, d_recv, l_sem, send2, recv2, send3, recv3):
    z = lax.axis_index("op")
    row = lax.axis_index("row")
    y, x, c = row // 8, (row // 2) % 4, row % 2
    nc = 1 - c
    along = x * nc + y * c
    across = y * nc + x * c
    slot_x = x * 2 + c
    slot_y = y * 2 + c

    def dev(yy, xx, cc):
        return yy * 8 + xx * 2 + cc

    def bytes_of(ref, sem):
        pltpu.make_async_copy(ref, ref, sem).wait()

    for p in range(PASSES):
        for s in range(8):
            rd[p, s, pl.ds(NR_LOC, 3)] = jnp.zeros((3, 2, ROWS, 128), BF16)

    barrier = pltpu.get_barrier_semaphore()

    def greet(zz, rr):
        pl.semaphore_signal(barrier, inc=1, device_id=(zz, rr), device_id_type=MESH)

    for j in (2, 1, 3):
        yy, xx, zz = (y + j) % 4, (x + j) % 4, (z + j) % 4
        near = dev(y * nc + yy * c, xx * nc + x * c, 0)
        greet(z, near)
        greet(z, near + 1)
        greet(z, dev(yy * nc + y * c, x * nc + xx * c, c))
        greet(zz, row)
    greet(z, dev(y, x, nc))

    base = (z % 2) * 8

    def data_src(tile, p, h):
        return ops_ref.at[z // 2, pl.ds(64 * h, SIZES[h]), :, tile, p]

    def data_dst(slot, p, h):
        return rd.at[p, slot, pl.ds(64 * h, SIZES[h])]

    def data_copy(slot, tile, p, h, target):
        return pltpu.make_async_remote_copy(
            src_ref=data_src(tile, p, h), dst_ref=data_dst(slot, p, h), send_sem=d_send,
            recv_sem=d_recv.at[slot // 2, p, h], device_id=target, device_id_type=MESH,
        )

    own_slot = along * 2 + c
    own_tile = base + c * 4 + along

    def own_data(p, h):
        return pltpu.make_async_copy(
            data_src(own_tile, p, h), data_dst(own_slot, p, h), d_recv.at[along, p, h]
        )

    kp_copy = pltpu.make_async_copy(kp_ref, kps, l_sem.at[0])
    v_copy = pltpu.make_async_copy(v_ref, vs_ref, l_sem.at[1])
    own_coord = pltpu.make_async_copy(coord_ref, rc.at[own_slot], c_recv)
    own_deg = pltpu.make_async_copy(deg_ref, rg.at[own_slot], g_recv)
    for copy in (kp_copy, own_coord, own_deg, v_copy):
        copy.start()
    for p in range(PASSES):
        for h in range(2):
            own_data(p, h).start()

    k_r, k_l = iota((256, 256), 0), iota((256, 256), 1)
    g_i, o32 = k_r // 64, (k_r // 2) % 32
    a_i = (o32 // 2) % 4
    owner = (o32 // 8) * 32 + o32 % 2 + (g_i * 8 + a_i * 2) * nc + (a_i * 8 + g_i * 2) * c
    pick[...] = jnp.where(k_l == owner * 2 + k_r % 2, 1.0, 0.0).astype(BF16)

    peers = []
    for j in (1, 3, 2):
        xx = (x + j) % 4
        yy = (y + j) % 4
        peers.append((slot_x, base + xx, (z, dev(y, xx, 0))))
        peers.append((slot_y, base + 4 + yy, (z, dev(yy, x, 1))))
    peers.append((slot_x * c + slot_y * nc, base + nc * 4 + x * c + y * nc, (z, dev(y, x, nc))))

    def coord_copy(slot, target):
        return pltpu.make_async_remote_copy(
            src_ref=coord_ref, dst_ref=rc.at[slot], send_sem=c_send,
            recv_sem=c_recv, device_id=target, device_id_type=MESH,
        )

    def deg_copy(slot, target):
        return pltpu.make_async_remote_copy(
            src_ref=deg_ref, dst_ref=rg.at[slot], send_sem=g_send,
            recv_sem=g_recv, device_id=target, device_id_type=MESH,
        )

    pl.semaphore_wait(barrier, 13)
    for slot, tile, target in peers:
        coord_copy(slot, target).start()
        deg_copy(slot, target).start()
    order = [(0, 0), (1, 0), (2, 0), (3, 0), (6, 0), (0, 1), (1, 1), (2, 1), (3, 1), (6, 1),
             (4, 0), (5, 0), (4, 1), (5, 1)]
    for p in range(PASSES):
        for k, h in order:
            slot, tile, target = peers[k]
            data_copy(slot, tile, p, h, target).start()

    o_i, i_i = iota((256, 256), 0), iota((256, 256), 1)
    p_o, p_i = iota((TALL, TALL), 0), iota((TALL, TALL), 1)
    perm[...] = jnp.where(p_i == (p_o % 64) * ROWS + p_o // 64, 1.0, 0.0).astype(BF16)

    kpp[...] = jnp.zeros(kpp.shape, F32)
    kp_copy.wait()
    kpp[0:3, :] = kps[...].astype(F32)
    kq[...] = nt(pick[...], kpp[...].astype(BF16)).astype(BF16)

    cm[...] = jnp.zeros(cm.shape, F32)
    rmat[...] = jnp.zeros(rmat.shape, BF16)
    bytes_of(rc, c_recv)
    bytes_of(rg, g_recv)
    for slot in range(8):
        at, lanes = (slot // 2) * 8, slice((slot % 2) * 128, (slot % 2) * 128 + NR_LOC)
        cm[at:at + 3, lanes] = rc[slot].astype(F32)
        cm[at + 3:at + 4, lanes] = rg[slot].astype(F32)
    s_c, s_h, s_r = (i_i % 128) // 64, i_i // 128, i_i % 64
    spread = jnp.where(o_i == s_c * 128 + s_h * 64 + s_r, 1.0, 0.0).astype(BF16)
    wx[...] = mm(cm[...].astype(BF16), spread)

    def turn_cos(u):
        u = u - ((u + MAGIC) - MAGIC)
        t = 0.25 - jnp.abs(u)
        q = t * t
        return t * (S0 + q * (S1 + q * (S2 + q * S3)))

    def phases(i, carry):
        chip, h = i // 2, i % 2
        blk = wx[pl.ds(pl.multiple_of(chip * 8, 8), 8), pl.ds(pl.multiple_of(h * 128, 128), 128)]
        deg = blk[3:4]
        weight = jnp.where(deg > 0.0, 1.0 / jnp.maximum(deg, 1.0), 0.0)
        place = blk[0:1] * 0.125
        rmat[0:16, :] = jnp.concatenate([blk * 0.0625, jnp.zeros((8, 128), F32)], axis=0).astype(BF16)

        for b in range(4):
            u = mm(kq[b * 64:(b + 1) * 64, :], rmat[...])
            cos = turn_cos(u) * weight
            sin = turn_cos(u - 0.25) * weight
            x_cos, x_sin = cos * place, sin * place
            for q, (first, second) in enumerate(((cos, -sin), (sin, cos), (-x_sin, -x_cos), (x_cos, -x_sin))):
                at = pl.ds(b * 256 + q, 64, stride=4)
                tw[0, at, :] = first
                tw[1, at, :] = second
        for b in range(4):
            rows = slice(b * 256, (b + 1) * 256)
            for part in range(2):
                ph[i, rows, part * 128:(part + 1) * 128] = tw[part, rows, :].astype(BF16)
        return carry

    lax.fori_loop(0, 8, phases, 0)

    def gather(p, i):
        off = jnp.where(i < 2, 0, jnp.where(i >= 6, 2, 1 + 2 * (i % 2)))
        h = jnp.where(i < 2, i, jnp.where(i < 4, 0, jnp.where(i < 6, 1, i - 6)))
        chip = (along + off) % 4
        for hh in range(2):
            @pl.when(h == hh)
            def _():
                bytes_of(rd.at[p, pl.ds(0, 2), pl.ds(0, SIZES[hh])], d_recv.at[chip, p, hh])

        at = pl.ds(h * 64, 64)
        blocks = [rd[p, chip * 2 + cc, at, part].reshape(TALL, 128) for part in range(2) for cc in range(2)]
        out = mm(perm[...], jnp.concatenate(blocks, axis=1)).astype(BF16)
        for n in range(4):
            for r in range(ROWS):
                tb[n * 64:(n + 1) * 64, r * 128:(r + 1) * 128] = out[r * 64:(r + 1) * 64, n * 128:(n + 1) * 128]
        return chip * 2 + h

    def partial_copy(t, g):
        yy, xx = g * nc + y * c, x * nc + g * c
        return pltpu.make_async_remote_copy(
            src_ref=sb.at[t, g], dst_ref=r2.at[t, across], send_sem=send2.at[t],
            recv_sem=recv2.at[t], device_id=(z, dev(yy, xx, c)), device_id_type=MESH,
        )

    groups = [(across + j) % 4 for j in (2, 1, 3)]

    def send_partials(t):
        for g in groups:
            partial_copy(t, g).start()

    for p in range(PASSES):
        acc[p] = jnp.zeros(acc.shape[1:], F32)

        def step(i, carry):
            at = gather(p, i)
            for n in range(WIDE // 256):
                cols = slice(n * 256, (n + 1) * 256)
                acc[p, :, cols] = acc[p, :, cols] + mm(ph[at], tb[:, cols])
            return carry

        lax.fori_loop(0, 7, step, 0)
        at = gather(p, 7)
        for t in range(p * PER, (p + 1) * PER):
            for n in range(SUB // 256):
                here = slice(n * 256, (n + 1) * 256)
                start = (t % PER) * SUB + n * 256
                cols = slice(start, start + 256)
                full = acc[p, :, cols] + mm(ph[at], tb[:, cols])
                acc[p, :, cols] = full
                sb[t, :, :, here] = full.reshape(4, 256, 256).astype(BF16)
            send_partials(t)

    def owner_copy(t, o, zz, aa, cc):
        yy, xx = y * nc + aa * c, aa * nc + x * c
        return pltpu.make_async_remote_copy(
            src_ref=s3.at[t, o], dst_ref=r3.at[t, my_slot], send_sem=send3.at[t],
            recv_sem=recv3.at[t], device_id=(zz, dev(yy, xx, cc)), device_id_type=MESH,
        )

    me_o = z * 8 + along * 2 + c
    my_slot = z * 8 + c * 4 + along

    def finish(t, b):
        rows = pl.ds(pl.multiple_of(across * 256 + b * 64, 64), 64)
        part = pl.ds(pl.multiple_of(b * 64, 64), 64)
        n = t % PER
        total = acc[t // PER, rows, n * SUB:(n + 1) * SUB]
        for g in groups:
            total = total + r2[t, g, part, :].astype(F32)
        s3[t, pl.ds(b * 8, 8)] = total.reshape(8, 8, SUB).astype(BF16)

    def send_block(t, b):
        for i in range(8):
            aa, cc = i // 2, i % 2
            o = b * 8 + i

            @pl.when(o != me_o)
            def _():
                owner_copy(t, o, b, aa, cc).start()

    def collect(t):
        bytes_of(r3.at[t], recv3.at[t])

        for slot in range(32):
            op, tile = slot // 16, slot % 16
            for r in range(SUB // 128):
                fs[pl.ds(op * 1024 + tile * 8 + (SUB // 128) * t + r, 8, stride=128), :] = r3[
                    t, slot, :, r * 128:(r + 1) * 128
                ].astype(F32)

    blocks = [(z + j) % 4 for j in (2, 1, 3, 0)]
    for t in range(SUBS):
        bytes_of(r2.at[t, pl.ds(0, 3)], recv2.at[t])
        for n, b in enumerate(blocks):
            finish(t, b)
            if n > 0:
                send_block(t, blocks[n - 1])
        send_block(t, blocks[3])
        pltpu.make_async_copy(s3.at[t, me_o], r3.at[t, my_slot], recv3.at[t]).start()
        if t >= LAG:
            collect(t - LAG)

    bytes_of(rc.at[pl.ds(0, 7)], c_send)
    bytes_of(rg.at[pl.ds(0, 7)], g_send)
    bytes_of(rd.at[:, pl.ds(0, 7), pl.ds(0, NR_LOC)], d_send)
    for t in range(SUBS):
        bytes_of(sb.at[t, pl.ds(0, 3)], send2.at[t])

    for t in range(max(SUBS - LAG, 0), SUBS):
        collect(t)

    v_copy.wait()
    def beside(*blocks):
        return jnp.concatenate(blocks, axis=1)

    def split(value):
        high = value.astype(BF16)
        return high, (value - high.astype(F32)).astype(BF16)

    lefts, stacks, fields = [], [], []
    for k2 in range(2):
        sums = []
        for j in range(4):
            for ri in range(2):
                at = ((j // 2) * 8 + k2 * 4 + (j % 2) * 2 + ri) * 128
                sums.append(fs[at:at + 128, :].astype(BF16))
        lefts.append(mm(vs_ref[k2].reshape(128, 128), beside(*sums)))
    for left in lefts:
        parts = []
        for j in range(4):
            lr = left[:, (2 * j) * 128:(2 * j + 1) * 128]
            li = left[:, (2 * j + 1) * 128:(2 * j + 2) * 128]
            parts.append(lr[:64] + li[64:])
            parts.append(li[:64] - lr[64:])
        stacks.append(jnp.concatenate(split(jnp.concatenate(parts, axis=0)), axis=0))
    for k2, stack in enumerate(stacks):
        yr, yi = nt(stack, vs_ref[k2, 0]), nt(stack, vs_ref[k2, 1])
        yr, yi = yr[:512] + yr[512:], yi[:512] + yi[512:]
        res = []
        for j in range(4):
            a, b = slice(128 * j, 128 * j + 64), slice(128 * j + 64, 128 * j + 128)
            res.append((yr[a] - yi[b], yi[a] + yr[b]))
        fields.append(res)
    for k2, ((hr, hi), (dr, di), (ar, ai), (er, ei)) in enumerate(fields):
        qr, qi = hr - di, hi + dr
        pr, pi = hr + di, hi - dr
        first = beside(ar, ai, pr, pi)
        second = jnp.concatenate([beside(qr, qi), beside(-qi, qr), beside(ar, ai), beside(-ai, ar)], axis=0)
        (f_high, f_low), (s_high, s_low) = split(first), split(second)
        both = mm(jnp.concatenate([f_high, f_low], axis=0), s_high)
        g[k2] = beside(er, ei) + FACTOR * (both[:64] + both[64:] + mm(f_high, s_low))
    for k2 in range(2):
        even, odd = g[k2, pl.ds(0, 32, stride=2), :], g[k2, pl.ds(1, 32, stride=2), :]
        og[k2, pl.ds(0, 32, stride=2), :] = beside(even[:, :64], odd[:, :64])
        og[k2, pl.ds(1, 32, stride=2), :] = beside(even[:, 64:], odd[:, 64:])
        pltpu.make_async_copy(og.at[k2], out_ref.at[k2], l_sem.at[0]).start()

    for t in range(SUBS):
        bytes_of(s3.at[t, pl.ds(0, 31)], send3.at[t])
    bytes_of(og, l_sem.at[0])


def on_device(wannier_ops, r_coords, degeneracy, kpoints, bloch_vectors):
    ops = wannier_ops.reshape(2, NR_LOC, 2, 16, PASSES, ROWS, 128)
    dma = pltpu.SemaphoreType.DMA
    vmem = pltpu.VMEM
    res = pl.pallas_call(
        kernel,
        out_shape=jax.ShapeDtypeStruct((2, 64, 128), F32),
        in_specs=[pl.BlockSpec(memory_space=pl.ANY)] * 5,
        out_specs=pl.BlockSpec(memory_space=pl.ANY),
        scratch_shapes=[
            vmem((8, 3, NR_LOC), I32),
            vmem((8, 1, NR_LOC), I32),
            vmem((PASSES, 8, 128, 2, ROWS, 128), BF16),
            vmem((3, 256), I32),
            vmem((2, 2, 64, 128), BF16),
            vmem((TALL, TALL), BF16),
            vmem((256, 256), BF16),
            vmem((128, 256), F32),
            vmem((256, 128), BF16),
            vmem((32, 256), F32),
            vmem((32, 256), F32),
            vmem((128, 128), BF16),
            vmem((2, 1024, 128), F32),
            vmem((8, 1024, 256), BF16),
            vmem((256, WIDE), BF16),
            vmem((PASSES, 1024, WIDE), F32),
            vmem((SUBS, 4, 256, SUB), BF16),
            vmem((SUBS, 4, 256, SUB), BF16),
            vmem((SUBS, 32, 8, SUB), BF16),
            vmem((SUBS, 32, 8, SUB), BF16),
            vmem((2048, 128), F32),
            vmem((2, 64, 128), F32),
            vmem((2, 64, 128), F32),
            dma, dma, dma, dma, dma, dma((4, PASSES, 2)), dma((2,)),
            dma((SUBS,)), dma((SUBS,)), dma((SUBS,)), dma((SUBS,)),
        ],
        compiler_params=pltpu.CompilerParams(
            collective_id=0, has_side_effects=True, vmem_limit_bytes=54 * 1024 * 1024
        ),
    )(r_coords.T, degeneracy.reshape(1, NR_LOC), kpoints.T, bloch_vectors, ops)
    return jnp.swapaxes(res.reshape(2, 32, 2, 128), 1, 2).reshape(2, 2, 4096)


def solution(mesh):
    in_specs = (
        P(None, "row", None, None, None),
        P("row", None),
        P("row"),
        P(),
        P(("op", "row"), None, None, None),
    )
    return jax.shard_map(
        on_device, mesh=mesh, in_specs=in_specs, out_specs=P(("op", "row"), None, None), check_vma=False
    )
```

```python
import jax
import jax.numpy as jnp
from jax import lax
from jax.experimental import pallas as pl
from jax.experimental.pallas import tpu as pltpu
from jax.sharding import PartitionSpec as P

MESH = pl.DeviceIdType.MESH
HIGH = lax.Precision.HIGHEST
F32 = jnp.float32
BF16 = jnp.bfloat16
I32 = jnp.int32

NR_LOC = 125
SIZES = (64, 61)
PASSES = 4
ROWS = 8 // PASSES
WIDE = ROWS * 128
TILES = WIDE // 256
SUB = 256
PER = WIDE // SUB
SUBS = PASSES * PER
LAG = 2 if SUBS > 2 else 1
VIA = 2
TALL = 64 * ROWS
FACTOR = 1.0 / 8.0
S0 = 0.392698743691337 * 16.0
S1 = -0.010092707352671412 * 16.0 ** 3
S2 = 7.766394538597307e-05 * 16.0 ** 5
S3 = -2.6791896176843414e-07 * 16.0 ** 7
MAGIC = 12582912.0


def nt(a, b, precision=None):
    return lax.dot_general(
        a, b, (((1,), (1,)), ((), ())), preferred_element_type=F32, precision=precision
    )


def mm(a, b, precision=None):
    return jnp.dot(a, b, preferred_element_type=F32, precision=precision)


def iota(shape, dim):
    return lax.broadcasted_iota(I32, shape, dim)


def kernel(coord_ref, deg_ref, kp_ref, v_ref, ops_ref, out_ref, rc, rg, rd, kps, vs_ref, perm, pick,
           kpp, kq, cm, wx, rmat, tw, ph, tb, acc, sb, r2, s3, r3, fs, g, og, far_in, far_out, c_send, c_recv, g_send, g_recv,
           d_send, d_recv, l_sem, send2, recv2, send3, recv3, send_f, recv_f, send_v):
    z = lax.axis_index("op")
    row = lax.axis_index("row")
    y, x, c = row // 8, (row // 2) % 4, row % 2
    nc = 1 - c
    along = x * nc + y * c
    across = y * nc + x * c
    slot_x = x * 2 + c
    slot_y = y * 2 + c

    def dev(yy, xx, cc):
        return yy * 8 + xx * 2 + cc

    def bytes_of(ref, sem):
        pltpu.make_async_copy(ref, ref, sem).wait()

    for p in range(PASSES):
        for s in range(8):
            rd[p, s, pl.ds(NR_LOC, 3)] = jnp.zeros((3, 2, ROWS, 128), BF16)

    barrier = pltpu.get_barrier_semaphore()

    def greet(zz, rr):
        pl.semaphore_signal(barrier, inc=1, device_id=(zz, rr), device_id_type=MESH)

    for j in (2, 1, 3):
        yy, xx, zz = (y + j) % 4, (x + j) % 4, (z + j) % 4
        near = dev(y * nc + yy * c, xx * nc + x * c, 0)
        greet(z, near)
        greet(z, near + 1)
        greet(z, dev(yy * nc + y * c, x * nc + xx * c, c))
        greet(zz, row)
    greet(z, dev(y, x, nc))

    base = (z % 2) * 8

    def data_src(tile, p, h):
        return ops_ref.at[z // 2, pl.ds(64 * h, SIZES[h]), :, tile, p]

    def data_dst(slot, p, h):
        return rd.at[p, slot, pl.ds(64 * h, SIZES[h])]

    def data_copy(slot, tile, p, h, target):
        return pltpu.make_async_remote_copy(
            src_ref=data_src(tile, p, h), dst_ref=data_dst(slot, p, h), send_sem=d_send,
            recv_sem=d_recv.at[slot // 2, p, h], device_id=target, device_id_type=MESH,
        )

    own_slot = along * 2 + c
    own_tile = base + c * 4 + along

    def own_data(p, h):
        return pltpu.make_async_copy(
            data_src(own_tile, p, h), data_dst(own_slot, p, h), d_recv.at[along, p, h]
        )

    kp_copy = pltpu.make_async_copy(kp_ref, kps, l_sem.at[0])
    v_copy = pltpu.make_async_copy(v_ref, vs_ref, l_sem.at[1])
    own_coord = pltpu.make_async_copy(coord_ref, rc.at[own_slot], c_recv)
    own_deg = pltpu.make_async_copy(deg_ref, rg.at[own_slot], g_recv)
    for copy in (kp_copy, own_coord, own_deg, v_copy):
        copy.start()
    for p in range(PASSES):
        for h in range(2):
            own_data(p, h).start()

    k_r, k_l = iota((256, 256), 0), iota((256, 256), 1)
    g_i, o32 = k_r // 64, (k_r // 2) % 32
    a_i = (o32 // 2) % 4
    owner = (o32 // 8) * 32 + o32 % 2 + (g_i * 8 + a_i * 2) * nc + (a_i * 8 + g_i * 2) * c
    pick[...] = jnp.where(k_l == owner * 2 + k_r % 2, 1.0, 0.0).astype(BF16)

    peers = []
    for j in (1, 3, 2):
        xx = (x + j) % 4
        yy = (y + j) % 4
        peers.append((slot_x, base + xx, (z, dev(y, xx, 0))))
        peers.append((slot_y, base + 4 + yy, (z, dev(yy, x, 1))))
    peers.append((slot_x * c + slot_y * nc, base + nc * 4 + x * c + y * nc, (z, dev(y, x, nc))))

    def coord_copy(slot, target):
        return pltpu.make_async_remote_copy(
            src_ref=coord_ref, dst_ref=rc.at[slot], send_sem=c_send,
            recv_sem=c_recv, device_id=target, device_id_type=MESH,
        )

    def deg_copy(slot, target):
        return pltpu.make_async_remote_copy(
            src_ref=deg_ref, dst_ref=rg.at[slot], send_sem=g_send,
            recv_sem=g_recv, device_id=target, device_id_type=MESH,
        )

    pl.semaphore_wait(barrier, 13)
    for slot, tile, target in peers:
        coord_copy(slot, target).start()
        deg_copy(slot, target).start()
    order = [(0, 0), (1, 0), (2, 0), (3, 0), (6, 0), (0, 1), (1, 1), (2, 1), (3, 1), (6, 1),
             (4, 0), (5, 0), (4, 1), (5, 1)]
    for p in range(PASSES):
        for k, h in order:
            slot, tile, target = peers[k]
            data_copy(slot, tile, p, h, target).start()

    o_i, i_i = iota((256, 256), 0), iota((256, 256), 1)
    p_o, p_i = iota((TALL, TALL), 0), iota((TALL, TALL), 1)
    perm[...] = jnp.where(p_i == (p_o % 64) * ROWS + p_o // 64, 1.0, 0.0).astype(BF16)

    kpp[...] = jnp.zeros(kpp.shape, F32)
    kp_copy.wait()
    kpp[0:3, :] = kps[...].astype(F32)
    kq[...] = nt(pick[...], kpp[...].astype(BF16)).astype(BF16)

    cm[...] = jnp.zeros(cm.shape, F32)
    rmat[...] = jnp.zeros(rmat.shape, BF16)
    bytes_of(rc, c_recv)
    bytes_of(rg, g_recv)
    for slot in range(8):
        at, lanes = (slot // 2) * 8, slice((slot % 2) * 128, (slot % 2) * 128 + NR_LOC)
        cm[at:at + 3, lanes] = rc[slot].astype(F32)
        cm[at + 3:at + 4, lanes] = rg[slot].astype(F32)
    s_c, s_h, s_r = (i_i % 128) // 64, i_i // 128, i_i % 64
    spread = jnp.where(o_i == s_c * 128 + s_h * 64 + s_r, 1.0, 0.0).astype(BF16)
    wx[...] = mm(cm[...].astype(BF16), spread)

    def turn_cos(u):
        u = u - ((u + MAGIC) - MAGIC)
        t = 0.25 - jnp.abs(u)
        q = t * t
        return t * (S0 + q * (S1 + q * (S2 + q * S3)))

    def phases(i, carry):
        chip, h = i // 2, i % 2
        blk = wx[pl.ds(pl.multiple_of(chip * 8, 8), 8), pl.ds(pl.multiple_of(h * 128, 128), 128)]
        deg = blk[3:4]
        weight = jnp.where(deg > 0.0, 1.0 / jnp.maximum(deg, 1.0), 0.0)
        place = blk[0:1] * 0.125
        rmat[0:16, :] = jnp.concatenate([blk * 0.0625, jnp.zeros((8, 128), F32)], axis=0).astype(BF16)

        for b in range(4):
            u = mm(kq[b * 64:(b + 1) * 64, :], rmat[...])
            cos = turn_cos(u) * weight
            sin = turn_cos(u - 0.25) * weight
            x_cos, x_sin = cos * place, sin * place
            for q, (first, second) in enumerate(((cos, -sin), (sin, cos), (-x_sin, -x_cos), (x_cos, -x_sin))):
                at = pl.ds(b * 256 + q, 64, stride=4)
                tw[0, at, :] = first
                tw[1, at, :] = second
        for b in range(4):
            rows = slice(b * 256, (b + 1) * 256)
            for part in range(2):
                ph[i, rows, part * 128:(part + 1) * 128] = tw[part, rows, :].astype(BF16)
        return carry

    lax.fori_loop(0, 8, phases, 0)

    def gather(p, i):
        off = jnp.where(i < 2, 0, jnp.where(i >= 6, 2, 1 + 2 * (i % 2)))
        h = jnp.where(i < 2, i, jnp.where(i < 4, 0, jnp.where(i < 6, 1, i - 6)))
        chip = (along + off) % 4
        for hh in range(2):
            @pl.when(h == hh)
            def _():
                bytes_of(rd.at[p, pl.ds(0, 2), pl.ds(0, SIZES[hh])], d_recv.at[chip, p, hh])

        at = pl.ds(h * 64, 64)
        blocks = [rd[p, chip * 2 + cc, at, part].reshape(TALL, 128) for part in range(2) for cc in range(2)]
        out = mm(perm[...], jnp.concatenate(blocks, axis=1)).astype(BF16)
        for n in range(4):
            for r in range(ROWS):
                tb[n * 64:(n + 1) * 64, r * 128:(r + 1) * 128] = out[r * 64:(r + 1) * 64, n * 128:(n + 1) * 128]
        return chip * 2 + h

    def partial_copy(t, g):
        yy, xx = g * nc + y * c, x * nc + g * c
        return pltpu.make_async_remote_copy(
            src_ref=sb.at[t, g], dst_ref=r2.at[t, across], send_sem=send2.at[t],
            recv_sem=recv2.at[t], device_id=(z, dev(yy, xx, c)), device_id_type=MESH,
        )

    groups = [(across + j) % 4 for j in (2, 1, 3)]

    def send_partials(t):
        for g in groups:
            partial_copy(t, g).start()

    def beside_me(d):
        return (across + 1 + 2 * d) % 4

    def line_copy(src, dst, sems, t, place):
        yy, xx = place * nc + y * c, x * nc + place * c
        return pltpu.make_async_remote_copy(
            src_ref=src, dst_ref=dst, send_sem=sems[0].at[t], recv_sem=sems[1].at[t],
            device_id=(z, dev(yy, xx, c)), device_id_type=MESH,
        )

    far = (across + 2) % 4

    def send_halves(t):
        for d in range(2):
            part = pl.ds(d * 128, 128)
            line_copy(sb.at[t, far, part], far_in.at[t, d], (send_f, recv_f), t, beside_me(d)).start()
        for d in range(2):
            part = pl.ds(d * 128, 128)
            near = beside_me(1 - d)
            line_copy(sb.at[t, near, part], r2.at[t, 0, part], (send2, recv2), t, near).start()

    def forward(t):
        bytes_of(far_in.at[t], recv_f.at[t])
        n = t % PER
        for d in range(2):
            rows = pl.ds(pl.multiple_of(beside_me(d) * 256 + d * 128, 128), 128)
            both = acc[t // PER, rows, n * SUB:(n + 1) * SUB] + far_in[t, d].astype(F32)
            far_out[t, d] = both.astype(BF16)
        for d in range(2):
            part = pl.ds(d * 128, 128)
            line_copy(far_out.at[t, d], r2.at[t, 1, part], (send_v, recv2), t, beside_me(d)).start()

    for p in range(PASSES):
        acc[p] = jnp.zeros(acc.shape[1:], F32)

        def step(i, carry):
            at = gather(p, i)
            for n in range(WIDE // 256):
                cols = slice(n * 256, (n + 1) * 256)
                acc[p, :, cols] = acc[p, :, cols] + mm(ph[at], tb[:, cols])
            return carry

        lax.fori_loop(0, 7, step, 0)
        if p == PASSES - 1:
            forward(0)
        at = gather(p, 7)
        for t in range(p * PER, (p + 1) * PER):
            for n in range(SUB // 256):
                here = slice(n * 256, (n + 1) * 256)
                start = (t % PER) * SUB + n * 256
                cols = slice(start, start + 256)
                full = acc[p, :, cols] + mm(ph[at], tb[:, cols])
                acc[p, :, cols] = full
                sb[t, :, :, here] = full.reshape(4, 256, 256).astype(BF16)
            if t < VIA:
                send_halves(t)
            elif t < SUBS - 1:
                send_partials(t)

    forward(1)
    send_partials(SUBS - 1)

    def owner_copy(t, o, zz, aa, cc):
        yy, xx = y * nc + aa * c, aa * nc + x * c
        return pltpu.make_async_remote_copy(
            src_ref=s3.at[t, o], dst_ref=r3.at[t, my_slot], send_sem=send3.at[t],
            recv_sem=recv3.at[t], device_id=(zz, dev(yy, xx, cc)), device_id_type=MESH,
        )

    me_o = z * 8 + along * 2 + c
    my_slot = z * 8 + c * 4 + along

    def finish(t, b):
        rows = pl.ds(pl.multiple_of(across * 256 + b * 64, 64), 64)
        part = pl.ds(pl.multiple_of(b * 64, 64), 64)
        n = t % PER
        total = acc[t // PER, rows, n * SUB:(n + 1) * SUB]
        for g in (groups if t >= VIA else (0, 1)):
            total = total + r2[t, g, part, :].astype(F32)
        s3[t, pl.ds(b * 8, 8)] = total.reshape(8, 8, SUB).astype(BF16)

    def send_block(t, b):
        for i in range(8):
            aa, cc = i // 2, i % 2
            o = b * 8 + i

            @pl.when(o != me_o)
            def _():
                owner_copy(t, o, b, aa, cc).start()

    def collect(t):
        bytes_of(r3.at[t], recv3.at[t])

        for slot in range(32):
            op, tile = slot // 16, slot % 16
            for r in range(SUB // 128):
                fs[pl.ds(op * 1024 + tile * 8 + (SUB // 128) * t + r, 8, stride=128), :] = r3[
                    t, slot, :, r * 128:(r + 1) * 128
                ].astype(F32)

    blocks = [(z + j) % 4 for j in (2, 1, 3, 0)]
    for t in range(SUBS):
        bytes_of(r2.at[t, pl.ds(0, 3 if t >= VIA else 2)], recv2.at[t])
        for n, b in enumerate(blocks):
            finish(t, b)
            if n > 0:
                send_block(t, blocks[n - 1])
        send_block(t, blocks[3])
        pltpu.make_async_copy(s3.at[t, me_o], r3.at[t, my_slot], recv3.at[t]).start()
        if t >= LAG:
            collect(t - LAG)

    bytes_of(rc.at[pl.ds(0, 7)], c_send)
    bytes_of(rg.at[pl.ds(0, 7)], g_send)
    bytes_of(rd.at[:, pl.ds(0, 7), pl.ds(0, NR_LOC)], d_send)
    for t in range(VIA):
        bytes_of(far_in.at[t], send_f.at[t])
        bytes_of(far_in.at[t], send2.at[t])
        bytes_of(far_out.at[t], send_v.at[t])
    for t in range(VIA, SUBS):
        bytes_of(sb.at[t, pl.ds(0, 3)], send2.at[t])

    for t in range(max(SUBS - LAG, 0), SUBS):
        collect(t)

    v_copy.wait()
    def beside(*blocks):
        return jnp.concatenate(blocks, axis=1)

    def split(value):
        high = value.astype(BF16)
        return high, (value - high.astype(F32)).astype(BF16)

    lefts, stacks, fields = [], [], []
    for k2 in range(2):
        sums = []
        for j in range(4):
            for ri in range(2):
                at = ((j // 2) * 8 + k2 * 4 + (j % 2) * 2 + ri) * 128
                sums.append(fs[at:at + 128, :].astype(BF16))
        lefts.append(mm(vs_ref[k2].reshape(128, 128), beside(*sums)))
    for left in lefts:
        parts = []
        for j in range(4):
            lr = left[:, (2 * j) * 128:(2 * j + 1) * 128]
            li = left[:, (2 * j + 1) * 128:(2 * j + 2) * 128]
            parts.append(lr[:64] + li[64:])
            parts.append(li[:64] - lr[64:])
        stacks.append(jnp.concatenate(split(jnp.concatenate(parts, axis=0)), axis=0))
    for k2, stack in enumerate(stacks):
        yr, yi = nt(stack, vs_ref[k2, 0]), nt(stack, vs_ref[k2, 1])
        yr, yi = yr[:512] + yr[512:], yi[:512] + yi[512:]
        res = []
        for j in range(4):
            a, b = slice(128 * j, 128 * j + 64), slice(128 * j + 64, 128 * j + 128)
            res.append((yr[a] - yi[b], yi[a] + yr[b]))
        fields.append(res)
    for k2, ((hr, hi), (dr, di), (ar, ai), (er, ei)) in enumerate(fields):
        qr, qi = hr - di, hi + dr
        pr, pi = hr + di, hi - dr
        first = beside(ar, ai, pr, pi)
        second = jnp.concatenate([beside(qr, qi), beside(-qi, qr), beside(ar, ai), beside(-ai, ar)], axis=0)
        (f_high, f_low), (s_high, s_low) = split(first), split(second)
        both = mm(jnp.concatenate([f_high, f_low], axis=0), s_high)
        g[k2] = beside(er, ei) + FACTOR * (both[:64] + both[64:] + mm(f_high, s_low))
    for k2 in range(2):
        even, odd = g[k2, pl.ds(0, 32, stride=2), :], g[k2, pl.ds(1, 32, stride=2), :]
        og[k2, pl.ds(0, 32, stride=2), :] = beside(even[:, :64], odd[:, :64])
        og[k2, pl.ds(1, 32, stride=2), :] = beside(even[:, 64:], odd[:, 64:])
        pltpu.make_async_copy(og.at[k2], out_ref.at[k2], l_sem.at[0]).start()

    for t in range(SUBS):
        bytes_of(s3.at[t, pl.ds(0, 31)], send3.at[t])
    bytes_of(og, l_sem.at[0])


def on_device(wannier_ops, r_coords, degeneracy, kpoints, bloch_vectors):
    ops = wannier_ops.reshape(2, NR_LOC, 2, 16, PASSES, ROWS, 128)
    dma = pltpu.SemaphoreType.DMA
    vmem = pltpu.VMEM
    res = pl.pallas_call(
        kernel,
        out_shape=jax.ShapeDtypeStruct((2, 64, 128), F32),
        in_specs=[pl.BlockSpec(memory_space=pl.ANY)] * 5,
        out_specs=pl.BlockSpec(memory_space=pl.ANY),
        scratch_shapes=[
            vmem((8, 3, NR_LOC), I32),
            vmem((8, 1, NR_LOC), I32),
            vmem((PASSES, 8, 128, 2, ROWS, 128), BF16),
            vmem((3, 256), I32),
            vmem((2, 2, 64, 128), BF16),
            vmem((TALL, TALL), BF16),
            vmem((256, 256), BF16),
            vmem((128, 256), F32),
            vmem((256, 128), BF16),
            vmem((32, 256), F32),
            vmem((32, 256), F32),
            vmem((128, 128), BF16),
            vmem((2, 1024, 128), F32),
            vmem((8, 1024, 256), BF16),
            vmem((256, WIDE), BF16),
            vmem((PASSES, 1024, WIDE), F32),
            vmem((SUBS, 4, 256, SUB), BF16),
            vmem((SUBS, 4, 256, SUB), BF16),
            vmem((SUBS, 32, 8, SUB), BF16),
            vmem((SUBS, 32, 8, SUB), BF16),
            vmem((2048, 128), F32),
            vmem((2, 64, 128), F32),
            vmem((2, 64, 128), F32),
            vmem((VIA, 2, 128, SUB), BF16),
            vmem((VIA, 2, 128, SUB), BF16),
            dma, dma, dma, dma, dma, dma((4, PASSES, 2)), dma((2,)),
            dma((SUBS,)), dma((SUBS,)), dma((SUBS,)), dma((SUBS,)), dma((VIA,)), dma((VIA,)), dma((VIA,)),
        ],
        compiler_params=pltpu.CompilerParams(
            collective_id=0, has_side_effects=True, vmem_limit_bytes=54 * 1024 * 1024
        ),
    )(r_coords.T, degeneracy.reshape(1, NR_LOC), kpoints.T, bloch_vectors, ops)
    return jnp.swapaxes(res.reshape(2, 32, 2, 128), 1, 2).reshape(2, 2, 4096)


def solution(mesh):
    in_specs = (
        P(None, "row", None, None, None),
        P("row", None),
        P("row"),
        P(),
        P(("op", "row"), None, None, None),
    )
    return jax.shard_map(
        on_device, mesh=mesh, in_specs=in_specs, out_specs=P(("op", "row"), None, None), check_vma=False
    )
```

```python
import jax
import jax.numpy as jnp
from jax import lax
from jax.experimental import pallas as pl
from jax.experimental.pallas import tpu as pltpu
from jax.sharding import PartitionSpec as P

MESH = pl.DeviceIdType.MESH
HIGH = lax.Precision.HIGHEST
F32 = jnp.float32
BF16 = jnp.bfloat16
I32 = jnp.int32

NR_LOC = 125
SIZES = (64, 61)
PASSES = 4
ROWS = 8 // PASSES
WIDE = ROWS * 128
TILES = WIDE // 256
SUB = 256
PER = WIDE // SUB
SUBS = PASSES * PER
LAG = SUBS
VIA = 2
TALL = 64 * ROWS
FACTOR = 1.0 / 8.0
S0 = 0.392698743691337 * 16.0
S1 = -0.010092707352671412 * 16.0 ** 3
S2 = 7.766394538597307e-05 * 16.0 ** 5
S3 = -2.6791896176843414e-07 * 16.0 ** 7
MAGIC = 12582912.0


def nt(a, b, precision=None):
    return lax.dot_general(
        a, b, (((1,), (1,)), ((), ())), preferred_element_type=F32, precision=precision
    )


def mm(a, b, precision=None):
    return jnp.dot(a, b, preferred_element_type=F32, precision=precision)


def iota(shape, dim):
    return lax.broadcasted_iota(I32, shape, dim)


def kernel(coord_ref, deg_ref, kp_ref, v_ref, ops_ref, out_ref, rc, rg, rd, kps, vs_ref, perm, pick,
           kpp, kq, cm, wx, rmat, tw, ph, tb, acc, sb, r2, s3, r3, fs, g, og, far_in, far_out, c_send, c_recv, g_send, g_recv,
           d_send, d_recv, l_sem, send2, recv2, send3, recv3, send_f, recv_f, send_v):
    z = lax.axis_index("op")
    row = lax.axis_index("row")
    y, x, c = row // 8, (row // 2) % 4, row % 2
    nc = 1 - c
    along = x * nc + y * c
    across = y * nc + x * c
    slot_x = x * 2 + c
    slot_y = y * 2 + c

    def dev(yy, xx, cc):
        return yy * 8 + xx * 2 + cc

    def bytes_of(ref, sem):
        pltpu.make_async_copy(ref, ref, sem).wait()

    barrier = pltpu.get_barrier_semaphore()

    def greet(zz, rr):
        pl.semaphore_signal(barrier, inc=1, device_id=(zz, rr), device_id_type=MESH)

    for j in (2, 1, 3):
        yy, xx, zz = (y + j) % 4, (x + j) % 4, (z + j) % 4
        near = dev(y * nc + yy * c, xx * nc + x * c, 0)
        greet(z, near)
        greet(z, near + 1)
        greet(z, dev(yy * nc + y * c, x * nc + xx * c, c))
        greet(zz, row)
    greet(z, dev(y, x, nc))

    base = (z % 2) * 8

    def data_src(tile, p, h):
        return ops_ref.at[z // 2, pl.ds(64 * h, SIZES[h]), :, tile, p]

    def data_dst(slot, p, h):
        return rd.at[p, slot, pl.ds(64 * h, SIZES[h])]

    def data_copy(slot, tile, p, h, target):
        return pltpu.make_async_remote_copy(
            src_ref=data_src(tile, p, h), dst_ref=data_dst(slot, p, h), send_sem=d_send,
            recv_sem=d_recv.at[slot // 2, p, h], device_id=target, device_id_type=MESH,
        )

    own_slot = along * 2 + c
    own_tile = base + c * 4 + along

    def own_data(p, h):
        return pltpu.make_async_copy(
            data_src(own_tile, p, h), data_dst(own_slot, p, h), d_recv.at[along, p, h]
        )

    kp_copy = pltpu.make_async_copy(kp_ref, kps, l_sem.at[0])
    v_copy = pltpu.make_async_copy(v_ref, vs_ref, l_sem.at[1])
    own_coord = pltpu.make_async_copy(coord_ref, rc.at[own_slot], c_recv)
    own_deg = pltpu.make_async_copy(deg_ref, rg.at[own_slot], g_recv)
    for copy in (kp_copy, own_coord, own_deg, v_copy):
        copy.start()
    for p in range(PASSES):
        for h in range(2):
            own_data(p, h).start()

    k_r, k_l = iota((256, 256), 0), iota((256, 256), 1)
    g_i, o32 = k_r // 64, (k_r // 2) % 32
    a_i = (o32 // 2) % 4
    owner = (o32 // 8) * 32 + o32 % 2 + (g_i * 8 + a_i * 2) * nc + (a_i * 8 + g_i * 2) * c
    pick[...] = jnp.where(k_l == owner * 2 + k_r % 2, 1.0, 0.0).astype(BF16)

    peers = []
    for j in (1, 3, 2):
        xx = (x + j) % 4
        yy = (y + j) % 4
        peers.append((slot_x, base + xx, (z, dev(y, xx, 0))))
        peers.append((slot_y, base + 4 + yy, (z, dev(yy, x, 1))))
    peers.append((slot_x * c + slot_y * nc, base + nc * 4 + x * c + y * nc, (z, dev(y, x, nc))))

    def coord_copy(slot, target):
        return pltpu.make_async_remote_copy(
            src_ref=coord_ref, dst_ref=rc.at[slot], send_sem=c_send,
            recv_sem=c_recv, device_id=target, device_id_type=MESH,
        )

    def deg_copy(slot, target):
        return pltpu.make_async_remote_copy(
            src_ref=deg_ref, dst_ref=rg.at[slot], send_sem=g_send,
            recv_sem=g_recv, device_id=target, device_id_type=MESH,
        )

    pl.semaphore_wait(barrier, 13)
    for slot, tile, target in peers:
        coord_copy(slot, target).start()
        deg_copy(slot, target).start()
    order = [(0, 0), (1, 0), (2, 0), (3, 0), (6, 0), (0, 1), (1, 1), (2, 1), (3, 1), (6, 1),
             (4, 0), (5, 0), (4, 1), (5, 1)]
    for p in range(PASSES):
        for k, h in order:
            slot, tile, target = peers[k]
            data_copy(slot, tile, p, h, target).start()

    for p in range(PASSES):
        for s in range(8):
            rd[p, s, pl.ds(NR_LOC, 3)] = jnp.zeros((3, 2, ROWS, 128), BF16)

    o_i, i_i = iota((256, 256), 0), iota((256, 256), 1)
    p_o, p_i = iota((TALL, TALL), 0), iota((TALL, TALL), 1)
    perm[...] = jnp.where(p_i == (p_o % 64) * ROWS + p_o // 64, 1.0, 0.0).astype(BF16)

    kpp[...] = jnp.zeros(kpp.shape, F32)
    kp_copy.wait()
    kpp[0:3, :] = kps[...].astype(F32)
    kq[...] = nt(pick[...], kpp[...].astype(BF16)).astype(BF16)

    cm[...] = jnp.zeros(cm.shape, F32)
    rmat[...] = jnp.zeros(rmat.shape, BF16)
    bytes_of(rc, c_recv)
    bytes_of(rg, g_recv)
    for slot in range(8):
        at, lanes = (slot // 2) * 8, slice((slot % 2) * 128, (slot % 2) * 128 + NR_LOC)
        cm[at:at + 3, lanes] = rc[slot].astype(F32)
        cm[at + 3:at + 4, lanes] = rg[slot].astype(F32)
    s_c, s_h, s_r = (i_i % 128) // 64, i_i // 128, i_i % 64
    spread = jnp.where(o_i == s_c * 128 + s_h * 64 + s_r, 1.0, 0.0).astype(BF16)
    wx[...] = mm(cm[...].astype(BF16), spread)

    def turn_cos(u):
        u = u - ((u + MAGIC) - MAGIC)
        t = 0.25 - jnp.abs(u)
        q = t * t
        return t * (S0 + q * (S1 + q * (S2 + q * S3)))

    def phases(i, carry):
        chip, h = i // 2, i % 2
        blk = wx[pl.ds(pl.multiple_of(chip * 8, 8), 8), pl.ds(pl.multiple_of(h * 128, 128), 128)]
        deg = blk[3:4]
        weight = jnp.where(deg > 0.0, 1.0 / jnp.maximum(deg, 1.0), 0.0)
        place = blk[0:1] * 0.125
        rmat[0:16, :] = jnp.concatenate([blk * 0.0625, jnp.zeros((8, 128), F32)], axis=0).astype(BF16)

        for b in range(4):
            u = mm(kq[b * 64:(b + 1) * 64, :], rmat[...])
            cos = turn_cos(u) * weight
            sin = turn_cos(u - 0.25) * weight
            x_cos, x_sin = cos * place, sin * place
            for q, (first, second) in enumerate(((cos, -sin), (sin, cos), (-x_sin, -x_cos), (x_cos, -x_sin))):
                at = pl.ds(b * 256 + q, 64, stride=4)
                tw[0, at, :] = first
                tw[1, at, :] = second
        for b in range(4):
            rows = slice(b * 256, (b + 1) * 256)
            for part in range(2):
                ph[i, rows, part * 128:(part + 1) * 128] = tw[part, rows, :].astype(BF16)
        return carry

    lax.fori_loop(0, 8, phases, 0)

    def gather(p, i):
        off = jnp.where(i < 2, 0, jnp.where(i >= 6, 2, 1 + 2 * (i % 2)))
        h = jnp.where(i < 2, i, jnp.where(i < 4, 0, jnp.where(i < 6, 1, i - 6)))
        chip = (along + off) % 4
        for hh in range(2):
            @pl.when(h == hh)
            def _():
                bytes_of(rd.at[p, pl.ds(0, 2), pl.ds(0, SIZES[hh])], d_recv.at[chip, p, hh])

        at = pl.ds(h * 64, 64)
        blocks = [rd[p, chip * 2 + cc, at, part].reshape(TALL, 128) for part in range(2) for cc in range(2)]
        out = mm(perm[...], jnp.concatenate(blocks, axis=1)).astype(BF16)
        for n in range(4):
            for r in range(ROWS):
                tb[n * 64:(n + 1) * 64, r * 128:(r + 1) * 128] = out[r * 64:(r + 1) * 64, n * 128:(n + 1) * 128]
        return chip * 2 + h

    def partial_copy(t, g):
        yy, xx = g * nc + y * c, x * nc + g * c
        return pltpu.make_async_remote_copy(
            src_ref=sb.at[t, g], dst_ref=r2.at[t, across], send_sem=send2.at[t],
            recv_sem=recv2.at[t], device_id=(z, dev(yy, xx, c)), device_id_type=MESH,
        )

    groups = [(across + j) % 4 for j in (2, 1, 3)]

    def send_partials(t):
        for g in groups:
            partial_copy(t, g).start()

    def beside_me(d):
        return (across + 1 + 2 * d) % 4

    def line_copy(src, dst, sems, t, place):
        yy, xx = place * nc + y * c, x * nc + place * c
        return pltpu.make_async_remote_copy(
            src_ref=src, dst_ref=dst, send_sem=sems[0].at[t], recv_sem=sems[1].at[t],
            device_id=(z, dev(yy, xx, c)), device_id_type=MESH,
        )

    far = (across + 2) % 4

    def send_halves(t):
        for d in range(2):
            part = pl.ds(d * 128, 128)
            line_copy(sb.at[t, far, part], far_in.at[t, d], (send_f, recv_f), t, beside_me(d)).start()
        for d in range(2):
            part = pl.ds(d * 128, 128)
            near = beside_me(1 - d)
            line_copy(sb.at[t, near, part], r2.at[t, 0, part], (send2, recv2), t, near).start()

    def forward(t):
        bytes_of(far_in.at[t], recv_f.at[t])
        n = t % PER
        for d in range(2):
            rows = pl.ds(pl.multiple_of(beside_me(d) * 256 + d * 128, 128), 128)
            both = acc[t // PER, rows, n * SUB:(n + 1) * SUB] + far_in[t, d].astype(F32)
            far_out[t, d] = both.astype(BF16)
        for d in range(2):
            part = pl.ds(d * 128, 128)
            line_copy(far_out.at[t, d], r2.at[t, 1, part], (send_v, recv2), t, beside_me(d)).start()

    for p in range(PASSES):
        acc[p] = jnp.zeros(acc.shape[1:], F32)

        def step(i, carry):
            at = gather(p, i)
            for n in range(WIDE // 256):
                cols = slice(n * 256, (n + 1) * 256)
                acc[p, :, cols] = acc[p, :, cols] + mm(ph[at], tb[:, cols])
            return carry

        lax.fori_loop(0, 7, step, 0)
        if p == PASSES - 1:
            forward(0)
        at = gather(p, 7)
        for t in range(p * PER, (p + 1) * PER):
            for n in range(SUB // 256):
                here = slice(n * 256, (n + 1) * 256)
                start = (t % PER) * SUB + n * 256
                cols = slice(start, start + 256)
                full = acc[p, :, cols] + mm(ph[at], tb[:, cols])
                acc[p, :, cols] = full
                sb[t, :, :, here] = full.reshape(4, 256, 256).astype(BF16)
            if t < VIA:
                send_halves(t)
            elif t < SUBS - 1:
                send_partials(t)

    forward(1)
    send_partials(SUBS - 1)

    def owner_copy(t, o, zz, aa, cc):
        yy, xx = y * nc + aa * c, aa * nc + x * c
        return pltpu.make_async_remote_copy(
            src_ref=s3.at[t, o], dst_ref=r3.at[t, my_slot], send_sem=send3.at[t],
            recv_sem=recv3.at[t], device_id=(zz, dev(yy, xx, cc)), device_id_type=MESH,
        )

    me_o = z * 8 + along * 2 + c
    my_slot = z * 8 + c * 4 + along

    def finish(t, b):
        rows = pl.ds(pl.multiple_of(across * 256 + b * 64, 64), 64)
        part = pl.ds(pl.multiple_of(b * 64, 64), 64)
        n = t % PER
        total = acc[t // PER, rows, n * SUB:(n + 1) * SUB]
        for g in (groups if t >= VIA else (0, 1)):
            total = total + r2[t, g, part, :].astype(F32)
        s3[t, pl.ds(b * 8, 8)] = total.reshape(8, 8, SUB).astype(BF16)

    def send_block(t, b):
        for i in range(8):
            aa, cc = i // 2, i % 2
            o = b * 8 + i

            @pl.when(o != me_o)
            def _():
                owner_copy(t, o, b, aa, cc).start()

    def collect(t):
        bytes_of(r3.at[t], recv3.at[t])

        for slot in range(32):
            op, tile = slot // 16, slot % 16
            for r in range(SUB // 128):
                fs[pl.ds(op * 1024 + tile * 8 + (SUB // 128) * t + r, 8, stride=128), :] = r3[
                    t, slot, :, r * 128:(r + 1) * 128
                ].astype(F32)

    blocks = [(z + j) % 4 for j in (2, 1, 3, 0)]
    for t in range(SUBS):
        bytes_of(r2.at[t, pl.ds(0, 3 if t >= VIA else 2)], recv2.at[t])
        for n, b in enumerate(blocks):
            finish(t, b)
            if n > 0:
                send_block(t, blocks[n - 1])
        send_block(t, blocks[3])
        pltpu.make_async_copy(s3.at[t, me_o], r3.at[t, my_slot], recv3.at[t]).start()
        if t >= LAG:
            collect(t - LAG)

    bytes_of(rc.at[pl.ds(0, 7)], c_send)
    bytes_of(rg.at[pl.ds(0, 7)], g_send)
    bytes_of(rd.at[:, pl.ds(0, 7), pl.ds(0, NR_LOC)], d_send)
    for t in range(VIA):
        bytes_of(far_in.at[t], send_f.at[t])
        bytes_of(far_in.at[t], send2.at[t])
        bytes_of(far_out.at[t], send_v.at[t])
    for t in range(VIA, SUBS):
        bytes_of(sb.at[t, pl.ds(0, 3)], send2.at[t])

    for t in range(max(SUBS - LAG, 0), SUBS):
        collect(t)

    v_copy.wait()
    def beside(*blocks):
        return jnp.concatenate(blocks, axis=1)

    def split(value):
        high = value.astype(BF16)
        return high, (value - high.astype(F32)).astype(BF16)

    lefts, stacks, fields = [], [], []
    for k2 in range(2):
        sums = []
        for j in range(4):
            for ri in range(2):
                at = ((j // 2) * 8 + k2 * 4 + (j % 2) * 2 + ri) * 128
                sums.append(fs[at:at + 128, :].astype(BF16))
        lefts.append(mm(vs_ref[k2].reshape(128, 128), beside(*sums)))
    for left in lefts:
        parts = []
        for j in range(4):
            lr = left[:, (2 * j) * 128:(2 * j + 1) * 128]
            li = left[:, (2 * j + 1) * 128:(2 * j + 2) * 128]
            parts.append(lr[:64] + li[64:])
            parts.append(li[:64] - lr[64:])
        stacks.append(jnp.concatenate(split(jnp.concatenate(parts, axis=0)), axis=0))
    for k2, stack in enumerate(stacks):
        yr, yi = nt(stack, vs_ref[k2, 0]), nt(stack, vs_ref[k2, 1])
        yr, yi = yr[:512] + yr[512:], yi[:512] + yi[512:]
        res = []
        for j in range(4):
            a, b = slice(128 * j, 128 * j + 64), slice(128 * j + 64, 128 * j + 128)
            res.append((yr[a] - yi[b], yi[a] + yr[b]))
        fields.append(res)
    for k2, ((hr, hi), (dr, di), (ar, ai), (er, ei)) in enumerate(fields):
        qr, qi = hr - di, hi + dr
        pr, pi = hr + di, hi - dr
        first = beside(ar, ai, pr, pi)
        second = jnp.concatenate([beside(qr, qi), beside(-qi, qr), beside(ar, ai), beside(-ai, ar)], axis=0)
        (f_high, f_low), (s_high, s_low) = split(first), split(second)
        both = mm(jnp.concatenate([f_high, f_low], axis=0), s_high)
        g[k2] = beside(er, ei) + FACTOR * (both[:64] + both[64:] + mm(f_high, s_low))
    for k2 in range(2):
        even, odd = g[k2, pl.ds(0, 32, stride=2), :], g[k2, pl.ds(1, 32, stride=2), :]
        og[k2, pl.ds(0, 32, stride=2), :] = beside(even[:, :64], odd[:, :64])
        og[k2, pl.ds(1, 32, stride=2), :] = beside(even[:, 64:], odd[:, 64:])
        pltpu.make_async_copy(og.at[k2], out_ref.at[k2], l_sem.at[0]).start()

    for t in range(SUBS):
        bytes_of(s3.at[t, pl.ds(0, 31)], send3.at[t])
    bytes_of(og, l_sem.at[0])


def on_device(wannier_ops, r_coords, degeneracy, kpoints, bloch_vectors):
    ops = wannier_ops.reshape(2, NR_LOC, 2, 16, PASSES, ROWS, 128)
    dma = pltpu.SemaphoreType.DMA
    vmem = pltpu.VMEM
    res = pl.pallas_call(
        kernel,
        out_shape=jax.ShapeDtypeStruct((2, 64, 128), F32),
        in_specs=[pl.BlockSpec(memory_space=pl.ANY)] * 5,
        out_specs=pl.BlockSpec(memory_space=pl.ANY),
        scratch_shapes=[
            vmem((8, 3, NR_LOC), I32),
            vmem((8, 1, NR_LOC), I32),
            vmem((PASSES, 8, 128, 2, ROWS, 128), BF16),
            vmem((3, 256), I32),
            vmem((2, 2, 64, 128), BF16),
            vmem((TALL, TALL), BF16),
            vmem((256, 256), BF16),
            vmem((128, 256), F32),
            vmem((256, 128), BF16),
            vmem((32, 256), F32),
            vmem((32, 256), F32),
            vmem((128, 128), BF16),
            vmem((2, 1024, 128), F32),
            vmem((8, 1024, 256), BF16),
            vmem((256, WIDE), BF16),
            vmem((PASSES, 1024, WIDE), F32),
            vmem((SUBS, 4, 256, SUB), BF16),
            vmem((SUBS, 4, 256, SUB), BF16),
            vmem((SUBS, 32, 8, SUB), BF16),
            vmem((SUBS, 32, 8, SUB), BF16),
            vmem((2048, 128), F32),
            vmem((2, 64, 128), F32),
            vmem((2, 64, 128), F32),
            vmem((VIA, 2, 128, SUB), BF16),
            vmem((VIA, 2, 128, SUB), BF16),
            dma, dma, dma, dma, dma, dma((4, PASSES, 2)), dma((2,)),
            dma((SUBS,)), dma((SUBS,)), dma((SUBS,)), dma((SUBS,)), dma((VIA,)), dma((VIA,)), dma((VIA,)),
        ],
        compiler_params=pltpu.CompilerParams(
            collective_id=0, has_side_effects=True, vmem_limit_bytes=54 * 1024 * 1024
        ),
    )(r_coords.T, degeneracy.reshape(1, NR_LOC), kpoints.T, bloch_vectors, ops)
    return jnp.swapaxes(res.reshape(2, 32, 2, 128), 1, 2).reshape(2, 2, 4096)


def solution(mesh):
    in_specs = (
        P(None, "row", None, None, None),
        P("row", None),
        P("row"),
        P(),
        P(("op", "row"), None, None, None),
    )
    return jax.shard_map(
        on_device, mesh=mesh, in_specs=in_specs, out_specs=P(("op", "row"), None, None), check_vma=False
    )
```

```python
import jax
import jax.numpy as jnp
from jax import lax
from jax.experimental import pallas as pl
from jax.experimental.pallas import tpu as pltpu
from jax.sharding import PartitionSpec as P

MESH = pl.DeviceIdType.MESH
HIGH = lax.Precision.HIGHEST
F32 = jnp.float32
BF16 = jnp.bfloat16
I32 = jnp.int32

NR_LOC = 125
SIZES = (64, 61)
PASSES = 4
ROWS = 8 // PASSES
WIDE = ROWS * 128
TILES = WIDE // 256
SUB = 256
PER = WIDE // SUB
SUBS = PASSES * PER
LAG = SUBS
VIA = 2
TALL = 64 * ROWS
FACTOR = 1.0 / 8.0
S0 = 0.392698743691337 * 16.0
S1 = -0.010092707352671412 * 16.0 ** 3
S2 = 7.766394538597307e-05 * 16.0 ** 5
S3 = -2.6791896176843414e-07 * 16.0 ** 7
MAGIC = 12582912.0


def nt(a, b, precision=None):
    return lax.dot_general(
        a, b, (((1,), (1,)), ((), ())), preferred_element_type=F32, precision=precision
    )


def mm(a, b, precision=None):
    return jnp.dot(a, b, preferred_element_type=F32, precision=precision)


def iota(shape, dim):
    return lax.broadcasted_iota(I32, shape, dim)


def kernel(coord_ref, deg_ref, kp_ref, v_ref, ops_ref, out_ref, rc, rg, rd, kps, vs_ref, perm, pick,
           kpp, kq, cm, wx, rmat, tw, ph, tb, acc, sb, r2, s3, r3, fs, g, og, far_in, far_out, c_send, c_recv, g_send, g_recv,
           d_send, d_recv, l_sem, send2, recv2, send3, recv3, send_f, recv_f, send_v):
    z = lax.axis_index("op")
    row = lax.axis_index("row")
    y, x, c = row // 8, (row // 2) % 4, row % 2
    nc = 1 - c
    along = x * nc + y * c
    across = y * nc + x * c
    slot_x = x * 2 + c
    slot_y = y * 2 + c

    def dev(yy, xx, cc):
        return yy * 8 + xx * 2 + cc

    def bytes_of(ref, sem):
        pltpu.make_async_copy(ref, ref, sem).wait()

    barrier = pltpu.get_barrier_semaphore()

    def greet(zz, rr):
        pl.semaphore_signal(barrier, inc=1, device_id=(zz, rr), device_id_type=MESH)

    for j in (2, 1, 3):
        yy, xx, zz = (y + j) % 4, (x + j) % 4, (z + j) % 4
        near = dev(y * nc + yy * c, xx * nc + x * c, 0)
        greet(z, near)
        greet(z, near + 1)
        greet(z, dev(yy * nc + y * c, x * nc + xx * c, c))
        greet(zz, row)
    greet(z, dev(y, x, nc))

    base = (z % 2) * 8

    def data_src(tile, p, h):
        return ops_ref.at[z // 2, pl.ds(64 * h, SIZES[h]), :, tile, p]

    def data_dst(slot, p, h):
        return rd.at[p, slot, pl.ds(64 * h, SIZES[h])]

    def data_copy(slot, tile, p, h, target):
        return pltpu.make_async_remote_copy(
            src_ref=data_src(tile, p, h), dst_ref=data_dst(slot, p, h), send_sem=d_send,
            recv_sem=d_recv.at[slot // 2, p, h], device_id=target, device_id_type=MESH,
        )

    own_slot = along * 2 + c
    own_tile = base + c * 4 + along

    def own_data(p, h):
        return pltpu.make_async_copy(
            data_src(own_tile, p, h), data_dst(own_slot, p, h), d_recv.at[along, p, h]
        )

    kp_copy = pltpu.make_async_copy(kp_ref, kps, l_sem.at[0])
    v_copy = pltpu.make_async_copy(v_ref, vs_ref, l_sem.at[1])
    own_coord = pltpu.make_async_copy(coord_ref, rc.at[own_slot], c_recv)
    own_deg = pltpu.make_async_copy(deg_ref, rg.at[own_slot], g_recv)
    for copy in (kp_copy, own_coord, own_deg, v_copy):
        copy.start()
    for p in range(PASSES):
        for h in range(2):
            own_data(p, h).start()

    k_r, k_l = iota((256, 256), 0), iota((256, 256), 1)
    g_i, o32 = k_r // 64, (k_r // 2) % 32
    a_i = (o32 // 2) % 4
    owner = (o32 // 8) * 32 + o32 % 2 + (g_i * 8 + a_i * 2) * nc + (a_i * 8 + g_i * 2) * c
    pick[...] = jnp.where(k_l == owner * 2 + k_r % 2, 1.0, 0.0).astype(BF16)

    peers = []
    for j in (1, 3, 2):
        xx = (x + j) % 4
        yy = (y + j) % 4
        peers.append((slot_x, base + xx, (z, dev(y, xx, 0))))
        peers.append((slot_y, base + 4 + yy, (z, dev(yy, x, 1))))
    peers.append((slot_x * c + slot_y * nc, base + nc * 4 + x * c + y * nc, (z, dev(y, x, nc))))

    def coord_copy(slot, target):
        return pltpu.make_async_remote_copy(
            src_ref=coord_ref, dst_ref=rc.at[slot], send_sem=c_send,
            recv_sem=c_recv, device_id=target, device_id_type=MESH,
        )

    def deg_copy(slot, target):
        return pltpu.make_async_remote_copy(
            src_ref=deg_ref, dst_ref=rg.at[slot], send_sem=g_send,
            recv_sem=g_recv, device_id=target, device_id_type=MESH,
        )

    pl.semaphore_wait(barrier, 13)
    for slot, tile, target in peers:
        coord_copy(slot, target).start()
        deg_copy(slot, target).start()
    order = [(0, 0), (1, 0), (2, 0), (3, 0), (6, 0), (0, 1), (1, 1), (2, 1), (3, 1), (6, 1),
             (4, 0), (5, 0), (4, 1), (5, 1)]
    for p in range(PASSES):
        for k, h in order:
            slot, tile, target = peers[k]
            data_copy(slot, tile, p, h, target).start()

    for p in range(PASSES):
        for s in range(8):
            rd[p, s, pl.ds(NR_LOC, 3)] = jnp.zeros((3, 2, ROWS, 128), BF16)

    o_i, i_i = iota((256, 256), 0), iota((256, 256), 1)
    p_o, p_i = iota((TALL, TALL), 0), iota((TALL, TALL), 1)
    perm[...] = jnp.where(p_i == (p_o % 64) * ROWS + p_o // 64, 1.0, 0.0).astype(BF16)

    kpp[...] = jnp.zeros(kpp.shape, F32)
    kp_copy.wait()
    kpp[0:3, :] = kps[...].astype(F32)
    kq[...] = nt(pick[...], kpp[...].astype(BF16)).astype(BF16)

    cm[...] = jnp.zeros(cm.shape, F32)
    rmat[...] = jnp.zeros(rmat.shape, BF16)
    bytes_of(rc, c_recv)
    bytes_of(rg, g_recv)
    for slot in range(8):
        at, lanes = (slot // 2) * 8, slice((slot % 2) * 128, (slot % 2) * 128 + NR_LOC)
        cm[at:at + 3, lanes] = rc[slot].astype(F32)
        cm[at + 3:at + 4, lanes] = rg[slot].astype(F32)
    s_c, s_h, s_r = (i_i % 128) // 64, i_i // 128, i_i % 64
    spread = jnp.where(o_i == s_c * 128 + s_h * 64 + s_r, 1.0, 0.0).astype(BF16)
    wx[...] = mm(cm[...].astype(BF16), spread)

    def turn_cos(u):
        u = u - ((u + MAGIC) - MAGIC)
        t = 0.25 - jnp.abs(u)
        q = t * t
        return t * (S0 + q * (S1 + q * (S2 + q * S3)))

    def phases(i, carry):
        chip, h = i // 2, i % 2
        blk = wx[pl.ds(pl.multiple_of(chip * 8, 8), 8), pl.ds(pl.multiple_of(h * 128, 128), 128)]
        deg = blk[3:4]
        weight = jnp.where(deg > 0.0, 1.0 / jnp.maximum(deg, 1.0), 0.0)
        place = blk[0:1] * 0.125
        rmat[0:16, :] = jnp.concatenate([blk * 0.0625, jnp.zeros((8, 128), F32)], axis=0).astype(BF16)

        for b in range(4):
            u = mm(kq[b * 64:(b + 1) * 64, :], rmat[...])
            cos = turn_cos(u) * weight
            sin = turn_cos(u - 0.25) * weight
            x_cos, x_sin = cos * place, sin * place
            for q, (first, second) in enumerate(((cos, -sin), (sin, cos), (-x_sin, -x_cos), (x_cos, -x_sin))):
                at = pl.ds(b * 256 + q, 64, stride=4)
                tw[0, at, :] = first
                tw[1, at, :] = second
        for b in range(4):
            rows = slice(b * 256, (b + 1) * 256)
            for part in range(2):
                ph[i, rows, part * 128:(part + 1) * 128] = tw[part, rows, :].astype(BF16)
        return carry

    lax.fori_loop(0, 8, phases, 0)

    def gather(p, i):
        off = jnp.where(i < 2, 0, jnp.where(i >= 6, 2, 1 + 2 * (i % 2)))
        h = jnp.where(i < 2, i, jnp.where(i < 4, 0, jnp.where(i < 6, 1, i - 6)))
        chip = (along + off) % 4
        for hh in range(2):
            @pl.when(h == hh)
            def _():
                bytes_of(rd.at[p, pl.ds(0, 2), pl.ds(0, SIZES[hh])], d_recv.at[chip, p, hh])

        at = pl.ds(h * 64, 64)
        blocks = [rd[p, chip * 2 + cc, at, part].reshape(TALL, 128) for part in range(2) for cc in range(2)]
        out = mm(perm[...], jnp.concatenate(blocks, axis=1)).astype(BF16)
        for n in range(4):
            for r in range(ROWS):
                tb[n * 64:(n + 1) * 64, r * 128:(r + 1) * 128] = out[r * 64:(r + 1) * 64, n * 128:(n + 1) * 128]
        return chip * 2 + h

    def partial_copy(t, g):
        yy, xx = g * nc + y * c, x * nc + g * c
        return pltpu.make_async_remote_copy(
            src_ref=sb.at[t, g], dst_ref=r2.at[t, across], send_sem=send2.at[t],
            recv_sem=recv2.at[t], device_id=(z, dev(yy, xx, c)), device_id_type=MESH,
        )

    groups = [(across + j) % 4 for j in (2, 1, 3)]

    def send_partials(t):
        for g in groups:
            partial_copy(t, g).start()

    def send_last():
        for half in range(2):
            part = pl.ds(half * 128, 128)
            for g in groups:
                yy, xx = g * nc + y * c, x * nc + g * c
                pltpu.make_async_remote_copy(
                    src_ref=sb.at[SUBS - 1, g, part], dst_ref=r2.at[SUBS - 1, across, part],
                    send_sem=send2.at[SUBS - 1], recv_sem=recv2.at[SUBS - 1 + half],
                    device_id=(z, dev(yy, xx, c)), device_id_type=MESH,
                ).start()

    def beside_me(d):
        return (across + 1 + 2 * d) % 4

    def line_copy(src, dst, sems, t, place):
        yy, xx = place * nc + y * c, x * nc + place * c
        return pltpu.make_async_remote_copy(
            src_ref=src, dst_ref=dst, send_sem=sems[0].at[t], recv_sem=sems[1].at[t],
            device_id=(z, dev(yy, xx, c)), device_id_type=MESH,
        )

    far = (across + 2) % 4

    def send_halves(t):
        for d in range(2):
            part = pl.ds(d * 128, 128)
            line_copy(sb.at[t, far, part], far_in.at[t, d], (send_f, recv_f), t, beside_me(d)).start()
        for d in range(2):
            part = pl.ds(d * 128, 128)
            near = beside_me(1 - d)
            line_copy(sb.at[t, near, part], r2.at[t, 0, part], (send2, recv2), t, near).start()

    def forward(t):
        bytes_of(far_in.at[t], recv_f.at[t])
        n = t % PER
        for d in range(2):
            rows = pl.ds(pl.multiple_of(beside_me(d) * 256 + d * 128, 128), 128)
            both = acc[t // PER, rows, n * SUB:(n + 1) * SUB] + far_in[t, d].astype(F32)
            far_out[t, d] = both.astype(BF16)
        for d in range(2):
            part = pl.ds(d * 128, 128)
            line_copy(far_out.at[t, d], r2.at[t, 1, part], (send_v, recv2), t, beside_me(d)).start()

    for p in range(PASSES):
        acc[p] = jnp.zeros(acc.shape[1:], F32)

        def step(i, carry):
            at = gather(p, i)
            for n in range(WIDE // 256):
                cols = slice(n * 256, (n + 1) * 256)
                acc[p, :, cols] = acc[p, :, cols] + mm(ph[at], tb[:, cols])
            return carry

        lax.fori_loop(0, 7, step, 0)
        if p == PASSES - 1:
            forward(0)
        at = gather(p, 7)
        for t in range(p * PER, (p + 1) * PER):
            for n in range(SUB // 256):
                here = slice(n * 256, (n + 1) * 256)
                start = (t % PER) * SUB + n * 256
                cols = slice(start, start + 256)
                full = acc[p, :, cols] + mm(ph[at], tb[:, cols])
                acc[p, :, cols] = full
                sb[t, :, :, here] = full.reshape(4, 256, 256).astype(BF16)
            if t < VIA:
                send_halves(t)
            elif t < SUBS - 1:
                send_partials(t)

    forward(1)
    send_last()

    def owner_copy(t, o, zz, aa, cc):
        yy, xx = y * nc + aa * c, aa * nc + x * c
        return pltpu.make_async_remote_copy(
            src_ref=s3.at[t, o], dst_ref=r3.at[t, my_slot], send_sem=send3.at[t],
            recv_sem=recv3.at[t], device_id=(zz, dev(yy, xx, cc)), device_id_type=MESH,
        )

    me_o = z * 8 + along * 2 + c
    my_slot = z * 8 + c * 4 + along

    def finish(t, b):
        rows = pl.ds(pl.multiple_of(across * 256 + b * 64, 64), 64)
        part = pl.ds(b * 64 if isinstance(b, int) else pl.multiple_of(b * 64, 64), 64)
        n = t % PER
        total = acc[t // PER, rows, n * SUB:(n + 1) * SUB]
        for g in (groups if t >= VIA else (0, 1)):
            total = total + r2[t, g, part, :].astype(F32)
        s3[t, pl.ds(b * 8, 8)] = total.reshape(8, 8, SUB).astype(BF16)

    def send_block(t, b):
        for i in range(8):
            aa, cc = i // 2, i % 2
            o = b * 8 + i

            @pl.when(o != me_o)
            def _():
                owner_copy(t, o, b, aa, cc).start()

    def collect(t):
        bytes_of(r3.at[t], recv3.at[t])

        for slot in range(32):
            op, tile = slot // 16, slot % 16
            for r in range(SUB // 128):
                fs[pl.ds(op * 1024 + tile * 8 + (SUB // 128) * t + r, 8, stride=128), :] = r3[
                    t, slot, :, r * 128:(r + 1) * 128
                ].astype(F32)

    blocks = [(z + j) % 4 for j in (2, 1, 3, 0)]
    for t in range(SUBS):
        if t < SUBS - 1:
            bytes_of(r2.at[t, pl.ds(0, 3 if t >= VIA else 2)], recv2.at[t])
            for n, b in enumerate(blocks):
                finish(t, b)
                if n > 0:
                    send_block(t, blocks[n - 1])
            send_block(t, blocks[3])
        else:
            for half in range(2):
                bytes_of(r2.at[t, pl.ds(0, 3), pl.ds(half * 128, 128)], recv2.at[t + half])
                for b in (2 * half, 2 * half + 1):
                    finish(t, b)
                for b in (2 * half, 2 * half + 1):
                    send_block(t, b)
        pltpu.make_async_copy(s3.at[t, me_o], r3.at[t, my_slot], recv3.at[t]).start()
        if t >= LAG:
            collect(t - LAG)

    bytes_of(rc.at[pl.ds(0, 7)], c_send)
    bytes_of(rg.at[pl.ds(0, 7)], g_send)
    bytes_of(rd.at[:, pl.ds(0, 7), pl.ds(0, NR_LOC)], d_send)
    for t in range(VIA):
        bytes_of(far_in.at[t], send_f.at[t])
        bytes_of(far_in.at[t], send2.at[t])
        bytes_of(far_out.at[t], send_v.at[t])
    for t in range(VIA, SUBS):
        bytes_of(sb.at[t, pl.ds(0, 3)], send2.at[t])

    for t in range(max(SUBS - LAG, 0), SUBS):
        collect(t)

    v_copy.wait()
    def beside(*blocks):
        return jnp.concatenate(blocks, axis=1)

    def split(value):
        high = value.astype(BF16)
        return high, (value - high.astype(F32)).astype(BF16)

    lefts, stacks, fields = [], [], []
    for k2 in range(2):
        sums = []
        for j in range(4):
            for ri in range(2):
                at = ((j // 2) * 8 + k2 * 4 + (j % 2) * 2 + ri) * 128
                sums.append(fs[at:at + 128, :].astype(BF16))
        lefts.append(mm(vs_ref[k2].reshape(128, 128), beside(*sums)))
    for left in lefts:
        parts = []
        for j in range(4):
            lr = left[:, (2 * j) * 128:(2 * j + 1) * 128]
            li = left[:, (2 * j + 1) * 128:(2 * j + 2) * 128]
            parts.append(lr[:64] + li[64:])
            parts.append(li[:64] - lr[64:])
        stacks.append(jnp.concatenate(split(jnp.concatenate(parts, axis=0)), axis=0))
    for k2, stack in enumerate(stacks):
        yr, yi = nt(stack, vs_ref[k2, 0]), nt(stack, vs_ref[k2, 1])
        yr, yi = yr[:512] + yr[512:], yi[:512] + yi[512:]
        res = []
        for j in range(4):
            a, b = slice(128 * j, 128 * j + 64), slice(128 * j + 64, 128 * j + 128)
            res.append((yr[a] - yi[b], yi[a] + yr[b]))
        fields.append(res)
    for k2, ((hr, hi), (dr, di), (ar, ai), (er, ei)) in enumerate(fields):
        qr, qi = hr - di, hi + dr
        pr, pi = hr + di, hi - dr
        first = beside(ar, ai, pr, pi)
        second = jnp.concatenate([beside(qr, qi), beside(-qi, qr), beside(ar, ai), beside(-ai, ar)], axis=0)
        (f_high, f_low), (s_high, s_low) = split(first), split(second)
        both = mm(jnp.concatenate([f_high, f_low], axis=0), s_high)
        g[k2] = beside(er, ei) + FACTOR * (both[:64] + both[64:] + mm(f_high, s_low))
    for k2 in range(2):
        even, odd = g[k2, pl.ds(0, 32, stride=2), :], g[k2, pl.ds(1, 32, stride=2), :]
        og[k2, pl.ds(0, 32, stride=2), :] = beside(even[:, :64], odd[:, :64])
        og[k2, pl.ds(1, 32, stride=2), :] = beside(even[:, 64:], odd[:, 64:])
        pltpu.make_async_copy(og.at[k2], out_ref.at[k2], l_sem.at[0]).start()

    for t in range(SUBS):
        bytes_of(s3.at[t, pl.ds(0, 31)], send3.at[t])
    bytes_of(og, l_sem.at[0])


def on_device(wannier_ops, r_coords, degeneracy, kpoints, bloch_vectors):
    ops = wannier_ops.reshape(2, NR_LOC, 2, 16, PASSES, ROWS, 128)
    dma = pltpu.SemaphoreType.DMA
    vmem = pltpu.VMEM
    res = pl.pallas_call(
        kernel,
        out_shape=jax.ShapeDtypeStruct((2, 64, 128), F32),
        in_specs=[pl.BlockSpec(memory_space=pl.ANY)] * 5,
        out_specs=pl.BlockSpec(memory_space=pl.ANY),
        scratch_shapes=[
            vmem((8, 3, NR_LOC), I32),
            vmem((8, 1, NR_LOC), I32),
            vmem((PASSES, 8, 128, 2, ROWS, 128), BF16),
            vmem((3, 256), I32),
            vmem((2, 2, 64, 128), BF16),
            vmem((TALL, TALL), BF16),
            vmem((256, 256), BF16),
            vmem((128, 256), F32),
            vmem((256, 128), BF16),
            vmem((32, 256), F32),
            vmem((32, 256), F32),
            vmem((128, 128), BF16),
            vmem((2, 1024, 128), F32),
            vmem((8, 1024, 256), BF16),
            vmem((256, WIDE), BF16),
            vmem((PASSES, 1024, WIDE), F32),
            vmem((SUBS, 4, 256, SUB), BF16),
            vmem((SUBS, 4, 256, SUB), BF16),
            vmem((SUBS, 32, 8, SUB), BF16),
            vmem((SUBS, 32, 8, SUB), BF16),
            vmem((2048, 128), F32),
            vmem((2, 64, 128), F32),
            vmem((2, 64, 128), F32),
            vmem((VIA, 2, 128, SUB), BF16),
            vmem((VIA, 2, 128, SUB), BF16),
            dma, dma, dma, dma, dma, dma((4, PASSES, 2)), dma((2,)),
            dma((SUBS,)), dma((SUBS + 1,)), dma((SUBS,)), dma((SUBS,)), dma((VIA,)), dma((VIA,)), dma((VIA,)),
        ],
        compiler_params=pltpu.CompilerParams(
            collective_id=0, has_side_effects=True, vmem_limit_bytes=54 * 1024 * 1024
        ),
    )(r_coords.T, degeneracy.reshape(1, NR_LOC), kpoints.T, bloch_vectors, ops)
    return jnp.swapaxes(res.reshape(2, 32, 2, 128), 1, 2).reshape(2, 2, 4096)


def solution(mesh):
    in_specs = (
        P(None, "row", None, None, None),
        P("row", None),
        P("row"),
        P(),
        P(("op", "row"), None, None, None),
    )
    return jax.shard_map(
        on_device, mesh=mesh, in_specs=in_specs, out_specs=P(("op", "row"), None, None), check_vma=False
    )
```

```python
import jax
import jax.numpy as jnp
from jax import lax
from jax.experimental import pallas as pl
from jax.experimental.pallas import tpu as pltpu
from jax.sharding import PartitionSpec as P

MESH = pl.DeviceIdType.MESH
HIGH = lax.Precision.HIGHEST
F32 = jnp.float32
BF16 = jnp.bfloat16
I32 = jnp.int32

NR_LOC = 125
SIZES = (64, 61)
PASSES = 4
ROWS = 8 // PASSES
WIDE = ROWS * 128
TILES = WIDE // 256
SUB = 256
PER = WIDE // SUB
SUBS = PASSES * PER
LAG = SUBS
VIA = 2
TALL = 64 * ROWS
FACTOR = 1.0 / 8.0
S0 = 0.392698743691337 * 16.0
S1 = -0.010092707352671412 * 16.0 ** 3
S2 = 7.766394538597307e-05 * 16.0 ** 5
S3 = -2.6791896176843414e-07 * 16.0 ** 7
MAGIC = 12582912.0


def nt(a, b, precision=None):
    return lax.dot_general(
        a, b, (((1,), (1,)), ((), ())), preferred_element_type=F32, precision=precision
    )


def mm(a, b, precision=None):
    return jnp.dot(a, b, preferred_element_type=F32, precision=precision)


def iota(shape, dim):
    return lax.broadcasted_iota(I32, shape, dim)


def kernel(coord_ref, deg_ref, kp_ref, v_ref, ops_ref, out_ref, rc, rg, rd, kps, vs_ref, perm, pick,
           kpp, kq, cm, wx, rmat, tw, ph, tb, acc, sb, r2, s3, r3, fs, g, og, far_in, far_out, c_send, c_recv, g_send, g_recv,
           d_send, d_recv, l_sem, send2, recv2, send3, recv3, send_f, recv_f, send_v):
    z = lax.axis_index("op")
    row = lax.axis_index("row")
    y, x, c = row // 8, (row // 2) % 4, row % 2
    nc = 1 - c
    along = x * nc + y * c
    across = y * nc + x * c
    slot_x = x * 2 + c
    slot_y = y * 2 + c

    def dev(yy, xx, cc):
        return yy * 8 + xx * 2 + cc

    def bytes_of(ref, sem):
        pltpu.make_async_copy(ref, ref, sem).wait()

    barrier = pltpu.get_barrier_semaphore()

    def greet(zz, rr):
        pl.semaphore_signal(barrier, inc=1, device_id=(zz, rr), device_id_type=MESH)

    for j in (2, 1, 3):
        yy, xx, zz = (y + j) % 4, (x + j) % 4, (z + j) % 4
        near = dev(y * nc + yy * c, xx * nc + x * c, 0)
        greet(z, near)
        greet(z, near + 1)
        greet(z, dev(yy * nc + y * c, x * nc + xx * c, c))
        greet(zz, row)
    greet(z, dev(y, x, nc))

    base = (z % 2) * 8

    def data_src(tile, p, h):
        return ops_ref.at[z // 2, pl.ds(64 * h, SIZES[h]), :, tile, p]

    def data_dst(slot, p, h):
        return rd.at[p, slot, pl.ds(64 * h, SIZES[h])]

    def data_copy(slot, tile, p, h, target):
        return pltpu.make_async_remote_copy(
            src_ref=data_src(tile, p, h), dst_ref=data_dst(slot, p, h), send_sem=d_send,
            recv_sem=d_recv.at[slot // 2, p, h], device_id=target, device_id_type=MESH,
        )

    own_slot = along * 2 + c
    own_tile = base + c * 4 + along

    def own_data(p, h):
        return pltpu.make_async_copy(
            data_src(own_tile, p, h), data_dst(own_slot, p, h), d_recv.at[along, p, h]
        )

    kp_copy = pltpu.make_async_copy(kp_ref, kps, l_sem.at[0])
    v_copy = pltpu.make_async_copy(v_ref, vs_ref, l_sem.at[1])
    own_coord = pltpu.make_async_copy(coord_ref, rc.at[own_slot], c_recv)
    own_deg = pltpu.make_async_copy(deg_ref, rg.at[own_slot], g_recv)
    for copy in (kp_copy, own_coord, own_deg, v_copy):
        copy.start()
    for p in range(PASSES):
        for h in range(2):
            own_data(p, h).start()

    k_r, k_l = iota((256, 256), 0), iota((256, 256), 1)
    g_i, o32 = k_r // 64, (k_r // 2) % 32
    a_i = (o32 // 2) % 4
    owner = (o32 // 8) * 32 + o32 % 2 + (g_i * 8 + a_i * 2) * nc + (a_i * 8 + g_i * 2) * c
    pick[...] = jnp.where(k_l == owner * 2 + k_r % 2, 1.0, 0.0).astype(BF16)

    peers = []
    for j in (1, 3, 2):
        xx = (x + j) % 4
        yy = (y + j) % 4
        peers.append((slot_x, base + xx, (z, dev(y, xx, 0))))
        peers.append((slot_y, base + 4 + yy, (z, dev(yy, x, 1))))
    peers.append((slot_x * c + slot_y * nc, base + nc * 4 + x * c + y * nc, (z, dev(y, x, nc))))

    def coord_copy(slot, target):
        return pltpu.make_async_remote_copy(
            src_ref=coord_ref, dst_ref=rc.at[slot], send_sem=c_send,
            recv_sem=c_recv, device_id=target, device_id_type=MESH,
        )

    def deg_copy(slot, target):
        return pltpu.make_async_remote_copy(
            src_ref=deg_ref, dst_ref=rg.at[slot], send_sem=g_send,
            recv_sem=g_recv, device_id=target, device_id_type=MESH,
        )

    pl.semaphore_wait(barrier, 13)
    for slot, tile, target in peers:
        coord_copy(slot, target).start()
        deg_copy(slot, target).start()
    order = [(0, 0), (1, 0), (2, 0), (3, 0), (6, 0), (0, 1), (1, 1), (2, 1), (3, 1), (6, 1),
             (4, 0), (5, 0), (4, 1), (5, 1)]
    for p in range(PASSES):
        for k, h in order:
            slot, tile, target = peers[k]
            data_copy(slot, tile, p, h, target).start()

    for p in range(PASSES):
        for s in range(8):
            rd[p, s, pl.ds(NR_LOC, 3)] = jnp.zeros((3, 2, ROWS, 128), BF16)

    o_i, i_i = iota((256, 256), 0), iota((256, 256), 1)
    p_o, p_i = iota((TALL, TALL), 0), iota((TALL, TALL), 1)
    perm[...] = jnp.where(p_i == (p_o % 64) * ROWS + p_o // 64, 1.0, 0.0).astype(BF16)

    kpp[...] = jnp.zeros(kpp.shape, F32)
    kp_copy.wait()
    kpp[0:3, :] = kps[...].astype(F32)
    kq[...] = nt(pick[...], kpp[...].astype(BF16)).astype(BF16)

    cm[...] = jnp.zeros(cm.shape, F32)
    rmat[...] = jnp.zeros(rmat.shape, BF16)
    bytes_of(rc, c_recv)
    bytes_of(rg, g_recv)
    for slot in range(8):
        at, lanes = (slot // 2) * 8, slice((slot % 2) * 128, (slot % 2) * 128 + NR_LOC)
        cm[at:at + 3, lanes] = rc[slot].astype(F32)
        cm[at + 3:at + 4, lanes] = rg[slot].astype(F32)
    s_c, s_h, s_r = (i_i % 128) // 64, i_i // 128, i_i % 64
    spread = jnp.where(o_i == s_c * 128 + s_h * 64 + s_r, 1.0, 0.0).astype(BF16)
    wx[...] = mm(cm[...].astype(BF16), spread)

    def turn_cos(u):
        u = u - ((u + MAGIC) - MAGIC)
        t = 0.25 - jnp.abs(u)
        q = t * t
        return t * (S0 + q * (S1 + q * (S2 + q * S3)))

    def phases(i, carry):
        chip, h = i // 2, i % 2
        blk = wx[pl.ds(pl.multiple_of(chip * 8, 8), 8), pl.ds(pl.multiple_of(h * 128, 128), 128)]
        deg = blk[3:4]
        weight = jnp.where(deg > 0.0, 1.0 / jnp.maximum(deg, 1.0), 0.0)
        place = blk[0:1] * 0.125
        rmat[0:16, :] = jnp.concatenate([blk * 0.0625, jnp.zeros((8, 128), F32)], axis=0).astype(BF16)

        for b in range(4):
            u = mm(kq[b * 64:(b + 1) * 64, :], rmat[...])
            cos = turn_cos(u) * weight
            sin = turn_cos(u - 0.25) * weight
            x_cos, x_sin = cos * place, sin * place
            for q, (first, second) in enumerate(((cos, -sin), (sin, cos), (-x_sin, -x_cos), (x_cos, -x_sin))):
                at = pl.ds(b * 256 + q, 64, stride=4)
                tw[0, at, :] = first
                tw[1, at, :] = second
        for b in range(4):
            rows = slice(b * 256, (b + 1) * 256)
            for part in range(2):
                ph[i, rows, part * 128:(part + 1) * 128] = tw[part, rows, :].astype(BF16)
        return carry

    lax.fori_loop(0, 8, phases, 0)

    def gather(p, i):
        off = jnp.where(i < 2, 0, jnp.where(i >= 6, 2, 1 + 2 * (i % 2)))
        h = jnp.where(i < 2, i, jnp.where(i < 4, 0, jnp.where(i < 6, 1, i - 6)))
        chip = (along + off) % 4
        for hh in range(2):
            @pl.when(h == hh)
            def _():
                bytes_of(rd.at[p, pl.ds(0, 2), pl.ds(0, SIZES[hh])], d_recv.at[chip, p, hh])

        at = pl.ds(h * 64, 64)
        blocks = [rd[p, chip * 2 + cc, at, part].reshape(TALL, 128) for part in range(2) for cc in range(2)]
        out = mm(perm[...], jnp.concatenate(blocks, axis=1)).astype(BF16)
        for n in range(4):
            for r in range(ROWS):
                tb[n * 64:(n + 1) * 64, r * 128:(r + 1) * 128] = out[r * 64:(r + 1) * 64, n * 128:(n + 1) * 128]
        return chip * 2 + h

    def partial_copy(t, g):
        yy, xx = g * nc + y * c, x * nc + g * c
        return pltpu.make_async_remote_copy(
            src_ref=sb.at[t, g], dst_ref=r2.at[t, across], send_sem=send2.at[t],
            recv_sem=recv2.at[t], device_id=(z, dev(yy, xx, c)), device_id_type=MESH,
        )

    groups = [(across + j) % 4 for j in (2, 1, 3)]

    def send_partials(t):
        for g in groups:
            partial_copy(t, g).start()

    def send_last():
        for quarter in range(4):
            part = pl.ds(quarter * 64, 64)
            for g in groups:
                yy, xx = g * nc + y * c, x * nc + g * c
                pltpu.make_async_remote_copy(
                    src_ref=sb.at[SUBS - 1, g, part], dst_ref=r2.at[SUBS - 1, across, part],
                    send_sem=send2.at[SUBS - 1], recv_sem=recv2.at[SUBS - 1 + quarter],
                    device_id=(z, dev(yy, xx, c)), device_id_type=MESH,
                ).start()

    def beside_me(d):
        return (across + 1 + 2 * d) % 4

    def line_copy(src, dst, sems, t, place):
        yy, xx = place * nc + y * c, x * nc + place * c
        return pltpu.make_async_remote_copy(
            src_ref=src, dst_ref=dst, send_sem=sems[0].at[t], recv_sem=sems[1].at[t],
            device_id=(z, dev(yy, xx, c)), device_id_type=MESH,
        )

    far = (across + 2) % 4

    def send_halves(t):
        for d in range(2):
            part = pl.ds(d * 128, 128)
            line_copy(sb.at[t, far, part], far_in.at[t, d], (send_f, recv_f), t, beside_me(d)).start()
        for d in range(2):
            part = pl.ds(d * 128, 128)
            near = beside_me(1 - d)
            line_copy(sb.at[t, near, part], r2.at[t, 0, part], (send2, recv2), t, near).start()

    def forward(t):
        bytes_of(far_in.at[t], recv_f.at[t])
        n = t % PER
        for d in range(2):
            rows = pl.ds(pl.multiple_of(beside_me(d) * 256 + d * 128, 128), 128)
            both = acc[t // PER, rows, n * SUB:(n + 1) * SUB] + far_in[t, d].astype(F32)
            far_out[t, d] = both.astype(BF16)
        for d in range(2):
            part = pl.ds(d * 128, 128)
            line_copy(far_out.at[t, d], r2.at[t, 1, part], (send_v, recv2), t, beside_me(d)).start()

    for p in range(PASSES):
        acc[p] = jnp.zeros(acc.shape[1:], F32)

        def step(i, carry):
            at = gather(p, i)
            for n in range(WIDE // 256):
                cols = slice(n * 256, (n + 1) * 256)
                acc[p, :, cols] = acc[p, :, cols] + mm(ph[at], tb[:, cols])
            return carry

        lax.fori_loop(0, 7, step, 0)
        if p == PASSES - 1:
            forward(0)
        at = gather(p, 7)
        for t in range(p * PER, (p + 1) * PER):
            for n in range(SUB // 256):
                here = slice(n * 256, (n + 1) * 256)
                start = (t % PER) * SUB + n * 256
                cols = slice(start, start + 256)
                full = acc[p, :, cols] + mm(ph[at], tb[:, cols])
                acc[p, :, cols] = full
                sb[t, :, :, here] = full.reshape(4, 256, 256).astype(BF16)
            if t < VIA:
                send_halves(t)
            elif t < SUBS - 1:
                send_partials(t)

    forward(1)
    send_last()

    def owner_copy(t, o, zz, aa, cc):
        yy, xx = y * nc + aa * c, aa * nc + x * c
        return pltpu.make_async_remote_copy(
            src_ref=s3.at[t, o], dst_ref=r3.at[t, my_slot], send_sem=send3.at[t],
            recv_sem=recv3.at[t], device_id=(zz, dev(yy, xx, cc)), device_id_type=MESH,
        )

    me_o = z * 8 + along * 2 + c
    my_slot = z * 8 + c * 4 + along

    def finish(t, b):
        rows = pl.ds(pl.multiple_of(across * 256 + b * 64, 64), 64)
        part = pl.ds(b * 64 if isinstance(b, int) else pl.multiple_of(b * 64, 64), 64)
        n = t % PER
        total = acc[t // PER, rows, n * SUB:(n + 1) * SUB]
        for g in (groups if t >= VIA else (0, 1)):
            total = total + r2[t, g, part, :].astype(F32)
        s3[t, pl.ds(b * 8, 8)] = total.reshape(8, 8, SUB).astype(BF16)

    def send_block(t, b):
        for i in range(8):
            aa, cc = i // 2, i % 2
            o = b * 8 + i

            @pl.when(o != me_o)
            def _():
                owner_copy(t, o, b, aa, cc).start()

    def collect(t):
        bytes_of(r3.at[t], recv3.at[t])

        for slot in range(32):
            op, tile = slot // 16, slot % 16
            for r in range(SUB // 128):
                fs[pl.ds(op * 1024 + tile * 8 + (SUB // 128) * t + r, 8, stride=128), :] = r3[
                    t, slot, :, r * 128:(r + 1) * 128
                ].astype(F32)

    blocks = [(z + j) % 4 for j in (2, 1, 3, 0)]
    for t in range(SUBS):
        if t < SUBS - 1:
            bytes_of(r2.at[t, pl.ds(0, 3 if t >= VIA else 2)], recv2.at[t])
            for n, b in enumerate(blocks):
                finish(t, b)
                if n > 0:
                    send_block(t, blocks[n - 1])
            send_block(t, blocks[3])
        else:
            for b in range(4):
                bytes_of(r2.at[t, pl.ds(0, 3), pl.ds(b * 64, 64)], recv2.at[t + b])
                finish(t, b)
                send_block(t, b)
        pltpu.make_async_copy(s3.at[t, me_o], r3.at[t, my_slot], recv3.at[t]).start()
        if t >= LAG:
            collect(t - LAG)

    bytes_of(rc.at[pl.ds(0, 7)], c_send)
    bytes_of(rg.at[pl.ds(0, 7)], g_send)
    bytes_of(rd.at[:, pl.ds(0, 7), pl.ds(0, NR_LOC)], d_send)
    for t in range(VIA):
        bytes_of(far_in.at[t], send_f.at[t])
        bytes_of(far_in.at[t], send2.at[t])
        bytes_of(far_out.at[t], send_v.at[t])
    for t in range(VIA, SUBS):
        bytes_of(sb.at[t, pl.ds(0, 3)], send2.at[t])

    for t in range(max(SUBS - LAG, 0), SUBS):
        collect(t)

    v_copy.wait()
    def beside(*blocks):
        return jnp.concatenate(blocks, axis=1)

    def split(value):
        high = value.astype(BF16)
        return high, (value - high.astype(F32)).astype(BF16)

    lefts, stacks, fields = [], [], []
    for k2 in range(2):
        sums = []
        for j in range(4):
            for ri in range(2):
                at = ((j // 2) * 8 + k2 * 4 + (j % 2) * 2 + ri) * 128
                sums.append(fs[at:at + 128, :].astype(BF16))
        lefts.append(mm(vs_ref[k2].reshape(128, 128), beside(*sums)))
    for left in lefts:
        parts = []
        for j in range(4):
            lr = left[:, (2 * j) * 128:(2 * j + 1) * 128]
            li = left[:, (2 * j + 1) * 128:(2 * j + 2) * 128]
            parts.append(lr[:64] + li[64:])
            parts.append(li[:64] - lr[64:])
        stacks.append(jnp.concatenate(split(jnp.concatenate(parts, axis=0)), axis=0))
    for k2, stack in enumerate(stacks):
        yr, yi = nt(stack, vs_ref[k2, 0]), nt(stack, vs_ref[k2, 1])
        yr, yi = yr[:512] + yr[512:], yi[:512] + yi[512:]
        res = []
        for j in range(4):
            a, b = slice(128 * j, 128 * j + 64), slice(128 * j + 64, 128 * j + 128)
            res.append((yr[a] - yi[b], yi[a] + yr[b]))
        fields.append(res)
    for k2, ((hr, hi), (dr, di), (ar, ai), (er, ei)) in enumerate(fields):
        qr, qi = hr - di, hi + dr
        pr, pi = hr + di, hi - dr
        first = beside(ar, ai, pr, pi)
        second = jnp.concatenate([beside(qr, qi), beside(-qi, qr), beside(ar, ai), beside(-ai, ar)], axis=0)
        (f_high, f_low), (s_high, s_low) = split(first), split(second)
        both = mm(jnp.concatenate([f_high, f_low], axis=0), s_high)
        g[k2] = beside(er, ei) + FACTOR * (both[:64] + both[64:] + mm(f_high, s_low))
    for k2 in range(2):
        even, odd = g[k2, pl.ds(0, 32, stride=2), :], g[k2, pl.ds(1, 32, stride=2), :]
        og[k2, pl.ds(0, 32, stride=2), :] = beside(even[:, :64], odd[:, :64])
        og[k2, pl.ds(1, 32, stride=2), :] = beside(even[:, 64:], odd[:, 64:])
        pltpu.make_async_copy(og.at[k2], out_ref.at[k2], l_sem.at[0]).start()

    for t in range(SUBS):
        bytes_of(s3.at[t, pl.ds(0, 31)], send3.at[t])
    bytes_of(og, l_sem.at[0])


def on_device(wannier_ops, r_coords, degeneracy, kpoints, bloch_vectors):
    ops = wannier_ops.reshape(2, NR_LOC, 2, 16, PASSES, ROWS, 128)
    dma = pltpu.SemaphoreType.DMA
    vmem = pltpu.VMEM
    res = pl.pallas_call(
        kernel,
        out_shape=jax.ShapeDtypeStruct((2, 64, 128), F32),
        in_specs=[pl.BlockSpec(memory_space=pl.ANY)] * 5,
        out_specs=pl.BlockSpec(memory_space=pl.ANY),
        scratch_shapes=[
            vmem((8, 3, NR_LOC), I32),
            vmem((8, 1, NR_LOC), I32),
            vmem((PASSES, 8, 128, 2, ROWS, 128), BF16),
            vmem((3, 256), I32),
            vmem((2, 2, 64, 128), BF16),
            vmem((TALL, TALL), BF16),
            vmem((256, 256), BF16),
            vmem((128, 256), F32),
            vmem((256, 128), BF16),
            vmem((32, 256), F32),
            vmem((32, 256), F32),
            vmem((128, 128), BF16),
            vmem((2, 1024, 128), F32),
            vmem((8, 1024, 256), BF16),
            vmem((256, WIDE), BF16),
            vmem((PASSES, 1024, WIDE), F32),
            vmem((SUBS, 4, 256, SUB), BF16),
            vmem((SUBS, 4, 256, SUB), BF16),
            vmem((SUBS, 32, 8, SUB), BF16),
            vmem((SUBS, 32, 8, SUB), BF16),
            vmem((2048, 128), F32),
            vmem((2, 64, 128), F32),
            vmem((2, 64, 128), F32),
            vmem((VIA, 2, 128, SUB), BF16),
            vmem((VIA, 2, 128, SUB), BF16),
            dma, dma, dma, dma, dma, dma((4, PASSES, 2)), dma((2,)),
            dma((SUBS,)), dma((SUBS + 3,)), dma((SUBS,)), dma((SUBS,)), dma((VIA,)), dma((VIA,)), dma((VIA,)),
        ],
        compiler_params=pltpu.CompilerParams(
            collective_id=0, has_side_effects=True, vmem_limit_bytes=54 * 1024 * 1024
        ),
    )(r_coords.T, degeneracy.reshape(1, NR_LOC), kpoints.T, bloch_vectors, ops)
    return jnp.swapaxes(res.reshape(2, 32, 2, 128), 1, 2).reshape(2, 2, 4096)


def solution(mesh):
    in_specs = (
        P(None, "row", None, None, None),
        P("row", None),
        P("row"),
        P(),
        P(("op", "row"), None, None, None),
    )
    return jax.shard_map(
        on_device, mesh=mesh, in_specs=in_specs, out_specs=P(("op", "row"), None, None), check_vma=False
    )
```
